512 devices in a mesh: section: 16 (over x_lo, y, core), shard: 32 (over z, x_hi).
Axes of the slice: x: 4 (x_hi: 2, x_lo: 2; x = x_hi * 2 + x_lo), y: 4, z: 16, core: 2. Of those that a mesh axis runs over, the one named last changes fastest.
Arguments:
- train_weights: float32 [16, 16384, 1024], P('section', 'shard'), may hold values from -0.046875 to 0.046875
- section_to_group: int32 [16], replicated, may hold values from 0 to 15, each once
- hidden: bfloat16 [2048, 16384], P(('section', 'shard')), may hold values from -6 to 6
- queries: bfloat16 [8192, 2048], P(('section', 'shard')), may hold values from -100 to 100
- kv_cache: bfloat16 [8192, 128, 256], P(('section', 'shard')), may hold values from -5 to 5
- lengths: int32 [2048], P('section'), may hold values from 2 to 127, as said below
Outputs:
- context: bfloat16 [8192, 2048], P(('section', 'shard'))
- layer_out: bfloat16 [16, 4, 256, 16384], P('section', None, 'shard')
The draws below stay inside these ranges and needn't reach their ends.
Inputs may be any that keep to these rules, and one draw needn't show every extreme that they name: `section_to_group`: a permutation: each rollout group runs exactly one trainer section's layer. `lengths`: every row has at least two cached tokens; some row of every device has 127.
All inputs are finite; a program needn't handle non-finite values.
Results may differ from the reference program's by a relative error of at most 0.006.
Values may be sent and summed in bfloat16 or wider, within the bound.
No kernel may reach another device: no remote copies, remote signals or barrier semaphores. Data moves between devices by JAX's collectives and lax.ppermute only.
A program may use at most 64 MiB of HBM per device.

```python
import math
import jax
import jax.numpy as jnp
from jax import lax

D = 16384
HD = 128
QPK = 16
KVH = 4
LEN = 128
ROWS = 128
KVC = 1024
N_SECTION = 16


def cache_values(key):
    entries = N_SECTION * KVH * ROWS
    drawn = jax.random.normal(jax.random.fold_in(key, 101), (entries, LEN, 2 * HD), jnp.float32)
    drawn = jnp.clip(drawn, -5.0, 5.0)
    return drawn


def draw_kv_cache(key, part):
    return cache_values(key).astype(jnp.bfloat16)


def draw_queries(key, part):
    entries = N_SECTION * KVH * ROWS
    drawn = jax.random.normal(jax.random.fold_in(key, 202), (entries, QPK * HD), jnp.float32)
    drawn = jnp.clip(drawn, -5.0, 5.0)
    return drawn.astype(jnp.bfloat16)


def draw_lengths(key, part):
    count = N_SECTION * ROWS
    drawn = jax.random.randint(jax.random.fold_in(key, 303), (count,), 2, LEN)
    return jnp.where(jnp.arange(count) % 5 == 0, LEN - 1, drawn).astype(jnp.int32)


def block_levels(stream_key, dims, shards, low, high):
    factor_of = 1.0
    for position, blocks in shards:
        draws = jax.random.uniform(jax.random.fold_in(jax.random.fold_in(stream_key, 6), position), (blocks,), jnp.float32, low / len(shards), high / len(shards))
        factor_of = factor_of * jnp.repeat(jnp.exp(draws), dims[position] // blocks).reshape((-1,) + (1,) * (len(dims) - 1 - position))
    return factor_of


def noise(stream_key, dims, deviation, reach, cuts=(), kind=jnp.bfloat16):
    values = deviation * jax.random.normal(stream_key, dims, jnp.float32)
    if cuts:
        values = values * block_levels(stream_key, dims, cuts, -0.22, 0.18)
    return jnp.clip(values, -reach, reach).astype(kind)


def setup_inputs(seed: int = 0) -> dict:
    arg_keys = jax.random.split(jax.random.key(seed), 7)
    return {
        "train_weights": noise(arg_keys[0], (N_SECTION, D, KVC), D ** -0.5, 0.046875, ((0, 16), (1, 32)), jnp.float32),
        "section_to_group": jax.random.permutation(arg_keys[1], N_SECTION).astype(jnp.int32),
        "hidden": noise(arg_keys[2], (N_SECTION * ROWS, D), 1.0, 6.0, ((0, 512),)),
        "queries": draw_queries(jax.random.fold_in(arg_keys[6], 71), 0),
        "kv_cache": draw_kv_cache(jax.random.fold_in(arg_keys[6], 71), 0),
        "lengths": draw_lengths(jax.random.fold_in(arg_keys[6], 71), 0),
    }


def attend(query_rows, cache_rows, fresh_rows, row_lengths):
    score_scale = 1.0 / math.sqrt(HD)
    query_f = query_rows.astype(jnp.float32)
    cached_keys = cache_rows[:, :, :HD].astype(jnp.float32)
    cached_values = cache_rows[:, :, HD:].astype(jnp.float32)
    key_new = fresh_rows[:, :HD].astype(jnp.float32)
    value_new = fresh_rows[:, HD:].astype(jnp.float32)
    scores = jnp.einsum('rhd,rtd->rht', query_f, cached_keys) * score_scale
    valid = jnp.arange(LEN)[None, None, :] < row_lengths[:, None, None]
    scores = jnp.where(valid, scores, -1e+30)
    fresh_score = jnp.einsum('rhd,rd->rh', query_f, key_new) * score_scale
    highest = jnp.maximum(lax.optimization_barrier(jnp.max(scores, axis=-1)), fresh_score)
    weights = jnp.where(valid, jnp.exp(scores - highest[..., None]), 0.0)
    fresh_weight = jnp.exp(fresh_score - highest)
    total = lax.optimization_barrier(jnp.sum(weights, axis=-1)) + fresh_weight
    probs = (weights / total[..., None]).astype(jnp.bfloat16)
    fresh_prob = (fresh_weight / total).astype(jnp.bfloat16)
    context = jnp.einsum('rht,rtd->rhd', probs.astype(jnp.float32), cached_values)
    context = context + fresh_prob.astype(jnp.float32)[..., None] * value_new[:, None, :]
    return context.reshape(context.shape[0], QPK * HD).astype(jnp.bfloat16)

def reference(train_weights, section_to_group, hidden, queries, kv_cache, lengths):
    source = jnp.argsort(section_to_group).astype(jnp.int32)

    def one_group(group_id):
        layer = lax.dynamic_index_in_dim(train_weights, source[group_id], 0, keepdims=False).astype(jnp.bfloat16)
        inputs = lax.dynamic_slice_in_dim(hidden, group_id * ROWS, ROWS, 0)
        fresh = jnp.dot(inputs, layer, preferred_element_type=jnp.float32).astype(jnp.bfloat16)
        fresh = fresh.reshape(ROWS, KVH, 2 * HD).transpose(1, 0, 2).reshape(KVH * ROWS, 2 * HD)
        query_rows = lax.dynamic_slice_in_dim(queries, group_id * KVH * ROWS, KVH * ROWS, 0).reshape(KVH * ROWS, QPK, HD)
        cache_rows = lax.dynamic_slice_in_dim(kv_cache, group_id * KVH * ROWS, KVH * ROWS, 0)
        row_lengths = jnp.tile(lax.dynamic_slice_in_dim(lengths, group_id * ROWS, ROWS, 0), KVH)
        kept = layer.reshape(D, KVH, 2 * HD).transpose(1, 2, 0)
        return (attend(query_rows, cache_rows, fresh, row_lengths), kept)
    result, layer_out = lax.map(one_group, jnp.arange(N_SECTION, dtype=jnp.int32))
    return (result.reshape(N_SECTION * KVH * ROWS, QPK * HD), layer_out)
```

```python
import math

import jax
import jax.numpy as jnp
from jax import lax
from jax.sharding import PartitionSpec as P

D = 16384
HD = 128
QPK = 16
KVH = 4
LEN = 128
ROWS = 128


def exchange(blocks, axis):
    return lax.all_to_all(blocks, axis, split_axis=0, concat_axis=0, tiled=True)


def attend(query_rows, cache_rows, fresh_rows, row_lengths):
    score_scale = 1.0 / math.sqrt(HD)
    cached_keys = cache_rows[:, :, :HD]
    cached_values = cache_rows[:, :, HD:]
    key_new = fresh_rows[:, :HD]
    value_new = fresh_rows[:, HD:]
    scores = (
        jnp.einsum("rhd,rtd->rht", query_rows, cached_keys, preferred_element_type=jnp.float32)
        * score_scale
    )
    valid = jnp.arange(LEN)[None, None, :] < row_lengths[:, None, None]
    scores = jnp.where(valid, scores, -1e30)
    fresh_score = (
        jnp.einsum("rhd,rd->rh", query_rows, key_new, preferred_element_type=jnp.float32)
        * score_scale
    )
    highest = jnp.maximum(jnp.max(scores, axis=-1), fresh_score)
    weights = jnp.where(valid, jnp.exp(scores - highest[..., None]), 0.0)
    fresh_weight = jnp.exp(fresh_score - highest)
    total = jnp.sum(weights, axis=-1) + fresh_weight
    probs = (weights / total[..., None]).astype(jnp.bfloat16)
    fresh_prob = (fresh_weight / total).astype(jnp.bfloat16)
    context = jnp.einsum("rht,rtd->rhd", probs, cached_values, preferred_element_type=jnp.float32)
    context = (
        context
        + fresh_prob.astype(jnp.float32)[..., None] * value_new.astype(jnp.float32)[:, None, :]
    )
    return context.reshape(context.shape[0], QPK * HD).astype(jnp.bfloat16)


def body(train_weights, section_to_group, hidden, queries, kv_cache, lengths):
    shards = lax.axis_size("shard")
    sections = lax.axis_size("section")
    per_head = shards // KVH
    row_block = ROWS // per_head
    piece_cols = 2 * HD // shards
    slice_rows = train_weights.shape[1]
    groups = jnp.arange(sections, dtype=jnp.int32)
    source = jnp.sum(
        jnp.where(section_to_group[None, :] == groups[:, None], groups[None, :], 0), axis=1
    )
    own = hidden.shape[0]
    inputs = exchange(hidden.reshape(own, shards, slice_rows).transpose(1, 0, 2), "shard")
    inputs = inputs.reshape(ROWS, slice_rows)
    flipped = train_weights[0].astype(jnp.bfloat16).T
    flipped = flipped.reshape(KVH, shards, piece_cols, slice_rows).transpose(1, 0, 2, 3)
    flipped = flipped.reshape(sections, -1, slice_rows)
    spread = exchange(flipped, "section")
    picked = spread.at[source].get(mode="promise_in_bounds")
    routed = exchange(picked, "section").reshape(shards, KVH, piece_cols, slice_rows)
    partial = lax.dot_general(
        inputs,
        routed.transpose(1, 0, 2, 3).reshape(KVH, 2 * HD, slice_rows),
        (((1,), (2,)), ((), ())),
        preferred_element_type=jnp.float32,
    )
    partial = partial.reshape(per_head, row_block, KVH, 2 * HD).transpose(2, 0, 1, 3)
    partial = exchange(partial.reshape(shards, row_block, 2 * HD), "shard")
    fresh = jnp.sum(partial, axis=0).astype(jnp.bfloat16)
    pieces = exchange(routed, "shard")
    layer_out = pieces.transpose(1, 2, 0, 3).reshape(1, KVH, piece_cols, D)
    block_index = lax.axis_index("shard") % per_head
    row_lengths = lax.dynamic_slice_in_dim(lengths, block_index * row_block, row_block, 0)
    query_rows = queries.reshape(row_block, QPK, HD)
    context = attend(query_rows, kv_cache, fresh, row_lengths)
    return (context, layer_out)


def solution(mesh):
    return jax.shard_map(
        body,
        mesh=mesh,
        in_specs=(
            P("section", "shard", None),
            P(),
            P(("section", "shard"), None),
            P(("section", "shard"), None),
            P(("section", "shard"), None, None),
            P("section"),
        ),
        out_specs=(P(("section", "shard"), None), P("section", None, "shard", None)),
        check_vma=False,
    )
```

```python
import math

import jax
import jax.numpy as jnp
from jax import lax
from jax.experimental import pallas as pl
from jax.experimental.pallas import tpu as pltpu
from jax.sharding import PartitionSpec as P

D = 16384
HD = 128
QPK = 16
KVH = 4
LEN = 128
ROWS = 128


def exchange(blocks, axis):
    return lax.all_to_all(blocks, axis, split_axis=0, concat_axis=0, tiled=True)


def attend(query_rows, cache_rows, fresh_rows, row_lengths):
    score_scale = 1.0 / math.sqrt(HD)
    cached_keys = cache_rows[:, :, :HD]
    cached_values = cache_rows[:, :, HD:]
    key_new = fresh_rows[:, :HD]
    value_new = fresh_rows[:, HD:]
    scores = (
        jnp.einsum("rhd,rtd->rht", query_rows, cached_keys, preferred_element_type=jnp.float32)
        * score_scale
    )
    valid = jnp.arange(LEN)[None, None, :] < row_lengths[:, None, None]
    scores = jnp.where(valid, scores, -1e30)
    fresh_score = (
        jnp.einsum("rhd,rd->rh", query_rows, key_new, preferred_element_type=jnp.float32)
        * score_scale
    )
    highest = jnp.maximum(jnp.max(scores, axis=-1), fresh_score)
    weights = jnp.where(valid, jnp.exp(scores - highest[..., None]), 0.0)
    fresh_weight = jnp.exp(fresh_score - highest)
    total = jnp.sum(weights, axis=-1) + fresh_weight
    probs = (weights / total[..., None]).astype(jnp.bfloat16)
    fresh_prob = (fresh_weight / total).astype(jnp.bfloat16)
    context = jnp.einsum("rht,rtd->rhd", probs, cached_values, preferred_element_type=jnp.float32)
    context = (
        context
        + fresh_prob.astype(jnp.float32)[..., None] * value_new.astype(jnp.float32)[:, None, :]
    )
    return context.reshape(context.shape[0], QPK * HD).astype(jnp.bfloat16)


def pack_kernel(inputs_ref, routed_ref, out_ref):
    head = pl.program_id(0)
    shards, _, piece, depth = routed_ref.shape
    half = piece
    per_head = shards // KVH
    block = routed_ref[:, 0]
    out_ref[:, :, pl.ds(pl.multiple_of(head * depth, depth), depth)] = block
    product = lax.dot_general(
        inputs_ref[...],
        block.reshape(2 * HD, depth),
        (((1,), (1,)), ((), ())),
        preferred_element_type=jnp.float32,
    )
    upper = product.astype(jnp.bfloat16)
    lower = (product[:, :HD] - upper[:, :HD].astype(jnp.float32)).astype(jnp.bfloat16)
    base = KVH * depth
    for i in range(per_head):
        for j in range(2):
            rows = slice((2 * i + j) * half, (2 * i + j + 1) * half)
            start = base + j * 2 * HD
            out_ref[pl.ds(head * per_head + i, 1), :, start : start + 2 * HD] = upper[rows][None]
            start = base + 4 * HD + j * HD
            out_ref[pl.ds(head * per_head + i, 1), :, start : start + HD] = lower[rows][None]


def pack(inputs, routed):
    shards, _, piece, depth = routed.shape
    width = KVH * depth + 6 * HD
    return pl.pallas_call(
        pack_kernel,
        grid=(KVH,),
        in_specs=[
            pl.BlockSpec((ROWS, depth), lambda h: (0, 0)),
            pl.BlockSpec((shards, 1, piece, depth), lambda h: (0, h, 0, 0)),
        ],
        out_specs=pl.BlockSpec((shards, piece, width), lambda h: (0, 0, 0)),
        out_shape=jax.ShapeDtypeStruct((shards, piece, width), jnp.bfloat16),
        cost_estimate=pl.CostEstimate(
            flops=2 * ROWS * KVH * 2 * HD * depth, bytes_accessed=3_000_000, transcendentals=0
        ),
    )(inputs, routed)


def body(train_weights, section_to_group, hidden, queries, kv_cache, lengths):
    shards = lax.axis_size("shard")
    sections = lax.axis_size("section")
    per_head = shards // KVH
    row_block = ROWS // per_head
    piece_cols = 2 * HD // shards
    slice_rows = train_weights.shape[1]
    groups = jnp.arange(sections, dtype=jnp.int32)
    source = jnp.sum(
        jnp.where(section_to_group[None, :] == groups[:, None], groups[None, :], 0), axis=1
    )
    own = hidden.shape[0]
    inputs = exchange(hidden.reshape(own, shards, slice_rows).transpose(1, 0, 2), "shard")
    inputs = inputs.reshape(ROWS, slice_rows)
    flipped = train_weights[0].astype(jnp.bfloat16).T
    flipped = flipped.reshape(KVH, shards, piece_cols, slice_rows).transpose(1, 0, 2, 3)
    flipped = flipped.reshape(sections, -1, slice_rows)
    spread = exchange(flipped, "section")
    picked = spread.at[source].get(mode="promise_in_bounds")
    routed = exchange(picked, "section").reshape(shards, KVH, piece_cols, slice_rows)
    received = exchange(pack(inputs, routed), "shard")
    base = KVH * slice_rows
    layer_out = received[:, :, :base].reshape(shards, piece_cols, KVH, slice_rows)
    layer_out = layer_out.transpose(2, 1, 0, 3).reshape(1, KVH, piece_cols, D)
    sums = jnp.sum(received[:, :, base:].astype(jnp.float32), axis=0)
    upper = jnp.concatenate([sums[:, : 2 * HD], sums[:, 2 * HD : 4 * HD]], axis=0)
    lower = jnp.concatenate([sums[:, 4 * HD : 5 * HD], sums[:, 5 * HD :]], axis=0)
    fresh = jnp.concatenate([upper[:, :HD] + lower, upper[:, HD:]], axis=1).astype(jnp.bfloat16)
    block_index = lax.axis_index("shard") % per_head
    row_lengths = lax.dynamic_slice_in_dim(lengths, block_index * row_block, row_block, 0)
    query_rows = queries.reshape(row_block, QPK, HD)
    context = attend(query_rows, kv_cache, fresh, row_lengths)
    return (context, layer_out)


def solution(mesh):
    return jax.shard_map(
        body,
        mesh=mesh,
        in_specs=(
            P("section", "shard", None),
            P(),
            P(("section", "shard"), None),
            P(("section", "shard"), None),
            P(("section", "shard"), None, None),
            P("section"),
        ),
        out_specs=(P(("section", "shard"), None), P("section", None, "shard", None)),
        check_vma=False,
    )
```

```python
import math

import jax
import jax.numpy as jnp
from jax import lax
from jax.experimental import pallas as pl
from jax.experimental.pallas import tpu as pltpu
from jax.sharding import PartitionSpec as P

D = 16384
HD = 128
QPK = 16
KVH = 4
LEN = 128
ROWS = 128


def exchange(blocks, axis):
    return lax.all_to_all(blocks, axis, split_axis=0, concat_axis=0, tiled=True)


def spread_rows(blocks):
    me = lax.axis_index("shard")
    shards = blocks.shape[0]

    def send(values, bits):
        return lax.ppermute(values, "shard", [(i, i ^ bits) for i in range(shards)])

    order = jnp.arange(shards, dtype=jnp.int32).reshape(4, 4, 2).transpose(1, 0, 2).reshape(-1)
    near = blocks.at[me ^ order].get(mode="promise_in_bounds")
    near = near.reshape((4, 4, 2) + blocks.shape[1:])
    with jax.named_scope("near"):
        near = [near[0]] + [send(near[k], k << 1) for k in range(1, 4)]
    far = [jnp.stack([v[k] for v in near]) for k in range(4)]
    with jax.named_scope("far"):
        far = [far[0]] + [send(far[k], k << 3) for k in range(1, 4)]
    same = jnp.stack([v[:, 0] for v in far])
    with jax.named_scope("side"):
        other = send(jnp.stack([v[:, 1] for v in far]), 1)
    merged = jnp.concatenate([same, other]).reshape((shards,) + blocks.shape[1:])
    relative = me ^ jnp.arange(shards, dtype=jnp.int32)
    place = (relative & 1) * (shards // 2) + (relative >> 1)
    return merged.at[place].get(mode="promise_in_bounds")


def attend(query_rows, cache_rows, fresh_rows, row_lengths):
    score_scale = 1.0 / math.sqrt(HD)
    cached_keys = cache_rows[:, :, :HD]
    cached_values = cache_rows[:, :, HD:]
    key_new = fresh_rows[:, :HD]
    value_new = fresh_rows[:, HD:]
    scores = (
        jnp.einsum("rhd,rtd->rht", query_rows, cached_keys, preferred_element_type=jnp.float32)
        * score_scale
    )
    valid = jnp.arange(LEN)[None, None, :] < row_lengths[:, None, None]
    scores = jnp.where(valid, scores, -1e30)
    fresh_score = (
        jnp.einsum("rhd,rd->rh", query_rows, key_new, preferred_element_type=jnp.float32)
        * score_scale
    )
    highest = jnp.maximum(jnp.max(scores, axis=-1), fresh_score)
    weights = jnp.where(valid, jnp.exp(scores - highest[..., None]), 0.0)
    fresh_weight = jnp.exp(fresh_score - highest)
    total = jnp.sum(weights, axis=-1) + fresh_weight
    probs = (weights / total[..., None]).astype(jnp.bfloat16)
    fresh_prob = (fresh_weight / total).astype(jnp.bfloat16)
    context = jnp.einsum("rht,rtd->rhd", probs, cached_values, preferred_element_type=jnp.float32)
    context = (
        context
        + fresh_prob.astype(jnp.float32)[..., None] * value_new.astype(jnp.float32)[:, None, :]
    )
    return context.reshape(context.shape[0], QPK * HD).astype(jnp.bfloat16)


def pack_kernel(inputs_ref, routed_ref, out_ref):
    head = pl.program_id(0)
    shards, _, piece, depth = routed_ref.shape
    half = piece
    per_head = shards // KVH
    block = routed_ref[:, 0]
    out_ref[:, :, pl.ds(pl.multiple_of(head * depth, depth), depth)] = block
    product = lax.dot_general(
        inputs_ref[...],
        block.reshape(2 * HD, depth),
        (((1,), (1,)), ((), ())),
        preferred_element_type=jnp.float32,
    )
    upper = product.astype(jnp.bfloat16)
    lower = (product[:, :HD] - upper[:, :HD].astype(jnp.float32)).astype(jnp.bfloat16)
    base = KVH * depth
    for i in range(per_head):
        for j in range(2):
            rows = slice((2 * i + j) * half, (2 * i + j + 1) * half)
            start = base + j * 2 * HD
            out_ref[pl.ds(head * per_head + i, 1), :, start : start + 2 * HD] = upper[rows][None]
            start = base + 4 * HD + j * HD
            out_ref[pl.ds(head * per_head + i, 1), :, start : start + HD] = lower[rows][None]


def pack(inputs, routed):
    shards, _, piece, depth = routed.shape
    width = KVH * depth + 6 * HD
    return pl.pallas_call(
        pack_kernel,
        grid=(KVH,),
        in_specs=[
            pl.BlockSpec((ROWS, depth), lambda h: (0, 0)),
            pl.BlockSpec((shards, 1, piece, depth), lambda h: (0, h, 0, 0)),
        ],
        out_specs=pl.BlockSpec((shards, piece, width), lambda h: (0, 0, 0)),
        out_shape=jax.ShapeDtypeStruct((shards, piece, width), jnp.bfloat16),
        cost_estimate=pl.CostEstimate(
            flops=2 * ROWS * KVH * 2 * HD * depth, bytes_accessed=3_000_000, transcendentals=0
        ),
    )(inputs, routed)


def body(train_weights, section_to_group, hidden, queries, kv_cache, lengths):
    shards = lax.axis_size("shard")
    sections = lax.axis_size("section")
    per_head = shards // KVH
    row_block = ROWS // per_head
    piece_cols = 2 * HD // shards
    slice_rows = train_weights.shape[1]
    groups = jnp.arange(sections, dtype=jnp.int32)
    source = jnp.sum(
        jnp.where(section_to_group[None, :] == groups[:, None], groups[None, :], 0), axis=1
    )
    own = hidden.shape[0]
    with jax.named_scope("rows"):
        inputs = spread_rows(hidden.reshape(own, shards, slice_rows).transpose(1, 0, 2))
    inputs = inputs.reshape(ROWS, slice_rows)
    flipped = train_weights[0].astype(jnp.bfloat16).T
    flipped = flipped.reshape(KVH, shards, piece_cols, slice_rows).transpose(1, 0, 2, 3)
    flipped = flipped.reshape(sections, -1, slice_rows)
    with jax.named_scope("first"):
        spread = exchange(flipped, "section")
    with jax.named_scope("pick"):
        picked = spread.at[source].get(mode="promise_in_bounds")
    with jax.named_scope("second"):
        routed = exchange(picked, "section").reshape(shards, KVH, piece_cols, slice_rows)
    received = exchange(pack(inputs, routed), "shard")
    base = KVH * slice_rows
    layer_out = received[:, :, :base].reshape(shards, piece_cols, KVH, slice_rows)
    layer_out = layer_out.transpose(2, 1, 0, 3).reshape(1, KVH, piece_cols, D)
    sums = jnp.sum(received[:, :, base:].astype(jnp.float32), axis=0)
    upper = jnp.concatenate([sums[:, : 2 * HD], sums[:, 2 * HD : 4 * HD]], axis=0)
    lower = jnp.concatenate([sums[:, 4 * HD : 5 * HD], sums[:, 5 * HD :]], axis=0)
    fresh = jnp.concatenate([upper[:, :HD] + lower, upper[:, HD:]], axis=1).astype(jnp.bfloat16)
    block_index = lax.axis_index("shard") % per_head
    row_lengths = lax.dynamic_slice_in_dim(lengths, block_index * row_block, row_block, 0)
    query_rows = queries.reshape(row_block, QPK, HD)
    context = attend(query_rows, kv_cache, fresh, row_lengths)
    return (context, layer_out)


def solution(mesh):
    return jax.shard_map(
        body,
        mesh=mesh,
        in_specs=(
            P("section", "shard", None),
            P(),
            P(("section", "shard"), None),
            P(("section", "shard"), None),
            P(("section", "shard"), None, None),
            P("section"),
        ),
        out_specs=(P(("section", "shard"), None), P("section", None, "shard", None)),
        check_vma=False,
    )
```

```python
import math

import jax
import jax.numpy as jnp
from jax import lax
from jax.experimental import pallas as pl
from jax.sharding import PartitionSpec as P


D = 16384
HD = 128
QPK = 16
KVH = 4
LEN = 128
ROWS = 128


def exchange(blocks, axis):
    return lax.all_to_all(blocks, axis, split_axis=0, concat_axis=0, tiled=True)


def spread_rows(blocks):
    me = lax.axis_index("shard")
    shards = blocks.shape[0]

    def send(values, bits):
        return lax.ppermute(values, "shard", [(i, i ^ bits) for i in range(shards)])

    order = jnp.arange(shards, dtype=jnp.int32).reshape(4, 4, 2).transpose(2, 1, 0).reshape(-1)
    start = blocks.at[me ^ order].get(mode="promise_in_bounds")
    start = start.reshape((2, 4, 4) + blocks.shape[1:])
    side = [start[0], send(start[1], 1)]
    near = [jnp.stack([v[k] for v in side]) for k in range(4)]
    near = [near[0]] + [send(near[k], k << 1) for k in range(1, 4)]
    far = [jnp.stack([v[:, k] for v in near]) for k in range(4)]
    far = [far[0]] + [send(far[k], k << 3) for k in range(1, 4)]
    merged = jnp.concatenate(far).reshape((shards,) + blocks.shape[1:])
    relative = me ^ jnp.arange(shards, dtype=jnp.int32)
    return merged.at[relative].get(mode="promise_in_bounds")


def attend(query_rows, cache_rows, fresh_rows, row_lengths):
    score_scale = 1.0 / math.sqrt(HD)
    cached_keys = cache_rows[:, :, :HD]
    cached_values = cache_rows[:, :, HD:]
    key_new = fresh_rows[:, :HD]
    value_new = fresh_rows[:, HD:]
    scores = (
        jnp.einsum("rhd,rtd->rht", query_rows, cached_keys, preferred_element_type=jnp.float32)
        * score_scale
    )
    valid = jnp.arange(LEN)[None, None, :] < row_lengths[:, None, None]
    scores = jnp.where(valid, scores, -1e30)
    fresh_score = (
        jnp.einsum("rhd,rd->rh", query_rows, key_new, preferred_element_type=jnp.float32)
        * score_scale
    )
    highest = jnp.maximum(jnp.max(scores, axis=-1), fresh_score)
    weights = jnp.where(valid, jnp.exp(scores - highest[..., None]), 0.0)
    fresh_weight = jnp.exp(fresh_score - highest)
    total = jnp.sum(weights, axis=-1) + fresh_weight
    probs = (weights / total[..., None]).astype(jnp.bfloat16)
    fresh_prob = (fresh_weight / total).astype(jnp.bfloat16)
    context = jnp.einsum("rht,rtd->rhd", probs, cached_values, preferred_element_type=jnp.float32)
    context = (
        context
        + fresh_prob.astype(jnp.float32)[..., None] * value_new.astype(jnp.float32)[:, None, :]
    )
    return context.reshape(context.shape[0], QPK * HD).astype(jnp.bfloat16)


def pack_kernel(inputs_ref, routed_ref, out_ref):
    head = pl.program_id(0)
    shards, _, piece, depth = routed_ref.shape
    half = piece
    per_head = shards // KVH
    block = routed_ref[:, 0]
    out_ref[:, :, pl.ds(pl.multiple_of(head * depth, depth), depth)] = block
    product = lax.dot_general(
        inputs_ref[...],
        block.reshape(2 * HD, depth),
        (((1,), (1,)), ((), ())),
        preferred_element_type=jnp.float32,
    )
    upper = product.astype(jnp.bfloat16)
    lower = (product[:, :HD] - upper[:, :HD].astype(jnp.float32)).astype(jnp.bfloat16)
    base = KVH * depth
    for i in range(per_head):
        for j in range(2):
            rows = slice((2 * i + j) * half, (2 * i + j + 1) * half)
            start = base + j * 2 * HD
            out_ref[pl.ds(head * per_head + i, 1), :, start : start + 2 * HD] = upper[rows][None]
            start = base + 4 * HD + j * HD
            out_ref[pl.ds(head * per_head + i, 1), :, start : start + HD] = lower[rows][None]


def pack(inputs, routed):
    shards, _, piece, depth = routed.shape
    width = KVH * depth + 6 * HD
    return pl.pallas_call(
        pack_kernel,
        grid=(KVH,),
        in_specs=[
            pl.BlockSpec((ROWS, depth), lambda h: (0, 0)),
            pl.BlockSpec((shards, 1, piece, depth), lambda h: (0, h, 0, 0)),
        ],
        out_specs=pl.BlockSpec((shards, piece, width), lambda h: (0, 0, 0)),
        out_shape=jax.ShapeDtypeStruct((shards, piece, width), jnp.bfloat16),
        cost_estimate=pl.CostEstimate(
            flops=2 * ROWS * KVH * 2 * HD * depth, bytes_accessed=3_000_000, transcendentals=0
        ),
    )(inputs, routed)


def step(train_weights, section_to_group, hidden, queries, kv_cache, lengths):
    shards = lax.axis_size("shard")
    sections = lax.axis_size("section")
    per_head = shards // KVH
    row_block = ROWS // per_head
    piece_cols = 2 * HD // shards
    slice_rows = train_weights.shape[1]
    groups = jnp.arange(sections, dtype=jnp.int32)
    source = jnp.sum(
        jnp.where(section_to_group[None, :] == groups[:, None], groups[None, :], 0), axis=1
    )
    own = hidden.shape[0]
    inputs = spread_rows(hidden.reshape(own, shards, slice_rows).transpose(1, 0, 2))
    inputs = inputs.reshape(ROWS, slice_rows)
    flipped = train_weights[0].astype(jnp.bfloat16).T
    flipped = flipped.reshape(KVH, shards, piece_cols, slice_rows).transpose(1, 0, 2, 3)
    flipped = flipped.reshape(sections, -1, slice_rows)
    spread = exchange(flipped, "section")
    picked = spread.at[source].get(mode="promise_in_bounds")
    routed = exchange(picked, "section").reshape(shards, KVH, piece_cols, slice_rows)
    received = exchange(pack(inputs, routed), "shard")
    base = KVH * slice_rows
    layer_out = received[:, :, :base].reshape(shards, piece_cols, KVH, slice_rows)
    layer_out = layer_out.transpose(2, 1, 0, 3).reshape(1, KVH, piece_cols, D)
    sums = jnp.sum(received[:, :, base:].astype(jnp.float32), axis=0)
    upper = jnp.concatenate([sums[:, : 2 * HD], sums[:, 2 * HD : 4 * HD]], axis=0)
    lower = jnp.concatenate([sums[:, 4 * HD : 5 * HD], sums[:, 5 * HD :]], axis=0)
    fresh = jnp.concatenate([upper[:, :HD] + lower, upper[:, HD:]], axis=1).astype(jnp.bfloat16)
    block_index = lax.axis_index("shard") % per_head
    row_lengths = lax.dynamic_slice_in_dim(lengths, block_index * row_block, row_block, 0)
    query_rows = queries.reshape(row_block, QPK, HD)
    context = attend(query_rows, kv_cache, fresh, row_lengths)
    return (context, layer_out)


def solution(mesh):
    return jax.shard_map(
        step,
        mesh=mesh,
        in_specs=(
            P("section", "shard", None),
            P(),
            P(("section", "shard"), None),
            P(("section", "shard"), None),
            P(("section", "shard"), None, None),
            P("section"),
        ),
        out_specs=(P(("section", "shard"), None), P("section", None, "shard", None)),
        check_vma=False,
    )
```

```python
import math

import jax
import jax.numpy as jnp
from jax import lax
from jax.experimental import pallas as pl
from jax.experimental.pallas import tpu as pltpu
from jax.sharding import PartitionSpec as P


D = 16384
HD = 128
QPK = 16
KVH = 4
LEN = 128
ROWS = 128


def exchange(blocks, axis):
    return lax.all_to_all(blocks, axis, split_axis=0, concat_axis=0, tiled=True)


def spread_rows(blocks):
    me = lax.axis_index("shard")
    shards = blocks.shape[0]

    def send(values, bits):
        return lax.ppermute(values, "shard", [(i, i ^ bits) for i in range(shards)])

    order = jnp.arange(shards, dtype=jnp.int32).reshape(4, 4, 2).transpose(2, 1, 0).reshape(-1)
    start = blocks.at[me ^ order].get(mode="promise_in_bounds")
    start = start.reshape((2, 4, 4) + blocks.shape[1:])
    side = [start[0], send(start[1], 1)]
    near = [jnp.stack([v[k] for v in side]) for k in range(4)]
    near = [near[0]] + [send(near[k], k << 1) for k in range(1, 4)]
    far = [jnp.stack([v[:, k] for v in near]) for k in range(4)]
    far = [far[0]] + [send(far[k], k << 3) for k in range(1, 4)]
    return jnp.concatenate(far).reshape((shards,) + blocks.shape[1:])


def attend(query_rows, cache_rows, fresh_rows, row_lengths):
    score_scale = 1.0 / math.sqrt(HD)
    cached_keys = cache_rows[:, :, :HD]
    cached_values = cache_rows[:, :, HD:]
    key_new = fresh_rows[:, :HD]
    value_new = fresh_rows[:, HD:]
    scores = (
        jnp.einsum("rhd,rtd->rht", query_rows, cached_keys, preferred_element_type=jnp.float32)
        * score_scale
    )
    valid = jnp.arange(LEN)[None, None, :] < row_lengths[:, None, None]
    scores = jnp.where(valid, scores, -1e30)
    fresh_score = (
        jnp.einsum("rhd,rd->rh", query_rows, key_new, preferred_element_type=jnp.float32)
        * score_scale
    )
    highest = jnp.maximum(jnp.max(scores, axis=-1), fresh_score)
    weights = jnp.where(valid, jnp.exp(scores - highest[..., None]), 0.0)
    fresh_weight = jnp.exp(fresh_score - highest)
    total = jnp.sum(weights, axis=-1) + fresh_weight
    probs = (weights / total[..., None]).astype(jnp.bfloat16)
    fresh_prob = (fresh_weight / total).astype(jnp.bfloat16)
    context = jnp.einsum("rht,rtd->rhd", probs, cached_values, preferred_element_type=jnp.float32)
    context = (
        context
        + fresh_prob.astype(jnp.float32)[..., None] * value_new.astype(jnp.float32)[:, None, :]
    )
    return context.reshape(context.shape[0], QPK * HD).astype(jnp.bfloat16)


VMEM = pl.BlockSpec(memory_space=pltpu.VMEM)


def flip_kernel(weights_ref, out_ref):
    step = pl.program_id(0)
    shards, heads, piece, _ = out_ref.shape
    rows = weights_ref.shape[1]
    lanes = pl.ds(pl.multiple_of(step * rows, rows), rows)
    for h in range(heads):
        width = shards * piece
        block = weights_ref[0, :, h * width : (h + 1) * width].astype(jnp.bfloat16)
        out_ref[:, h, :, lanes] = block.T.reshape(shards, piece, rows)


def flip(weights, shards):
    _, depth, columns = weights.shape
    piece = columns // KVH // shards
    rows = 128
    return pl.pallas_call(
        flip_kernel,
        grid=(depth // rows,),
        in_specs=[pl.BlockSpec((1, rows, columns), lambda i: (0, i, 0))],
        out_specs=VMEM,
        out_shape=jax.ShapeDtypeStruct((shards, KVH, piece, depth), jnp.bfloat16),
        cost_estimate=pl.CostEstimate(flops=2_000_000, bytes_accessed=3_000_000, transcendentals=0),
        compiler_params=pltpu.CompilerParams(vmem_limit_bytes=12 * 1024 * 1024),
        name="flip",
    )(weights)


def pick_kernel(group_ref, spread_ref, out_ref):
    def move(s, carry):
        out_ref[group_ref[s]] = spread_ref[s]
        return carry

    lax.fori_loop(0, spread_ref.shape[0], move, 0)


def pick(section_to_group, spread):
    return pl.pallas_call(
        pick_kernel,
        in_specs=[pl.BlockSpec(memory_space=pltpu.SMEM), VMEM],
        out_specs=VMEM,
        out_shape=jax.ShapeDtypeStruct(spread.shape, spread.dtype),
        cost_estimate=pl.CostEstimate(flops=1_000_000, bytes_accessed=2_000_000, transcendentals=0),
        compiler_params=pltpu.CompilerParams(vmem_limit_bytes=12 * 1024 * 1024),
        name="pick",
    )(section_to_group, spread)


def pack_kernel(me_ref, inputs_ref, routed_ref, out_ref, rows_ref):
    me = me_ref[0]
    shards, heads, piece, depth = routed_ref.shape
    per_head = shards // heads
    own = inputs_ref.shape[1]
    for d in range(shards):
        rows_ref[d * own : (d + 1) * own, :] = inputs_ref[me ^ d].astype(jnp.float32)
    inputs = rows_ref[...].astype(jnp.bfloat16)
    base = heads * depth
    for h in range(heads):
        block = routed_ref[:, h]
        out_ref[:, :, h * depth : (h + 1) * depth] = block
        product = lax.dot_general(
            inputs,
            block.reshape(shards * piece, depth),
            (((1,), (1,)), ((), ())),
            preferred_element_type=jnp.float32,
        )
        upper = product.astype(jnp.bfloat16)
        lower = (product[:, :HD] - upper[:, :HD].astype(jnp.float32)).astype(jnp.bfloat16)
        for i in range(per_head):
            for j in range(2):
                rows = slice((2 * i + j) * piece, (2 * i + j + 1) * piece)
                start = base + j * 2 * HD
                out_ref[h * per_head + i, :, start : start + 2 * HD] = upper[rows]
                start = base + 4 * HD + j * HD
                out_ref[h * per_head + i, :, start : start + HD] = lower[rows]


def pack(me, inputs, routed):
    shards, heads, piece, depth = routed.shape
    width = heads * depth + 6 * HD
    return pl.pallas_call(
        pack_kernel,
        in_specs=[pl.BlockSpec(memory_space=pltpu.SMEM), VMEM, VMEM],
        out_specs=VMEM,
        out_shape=jax.ShapeDtypeStruct((shards, piece, width), jnp.bfloat16),
        scratch_shapes=[pltpu.VMEM((ROWS, depth), jnp.float32)],
        cost_estimate=pl.CostEstimate(
            flops=2 * ROWS * heads * 2 * HD * depth, bytes_accessed=3_000_000, transcendentals=0
        ),
        compiler_params=pltpu.CompilerParams(vmem_limit_bytes=12 * 1024 * 1024),
        name="pack",
    )(me, inputs, routed)


def step(train_weights, section_to_group, hidden, queries, kv_cache, lengths):
    shards = lax.axis_size("shard")
    sections = lax.axis_size("section")
    per_head = shards // KVH
    row_block = ROWS // per_head
    piece_cols = 2 * HD // shards
    slice_rows = train_weights.shape[1]
    own = hidden.shape[0]
    inputs = spread_rows(hidden.reshape(own, shards, slice_rows).transpose(1, 0, 2))
    flipped = flip(train_weights, shards).reshape(sections, -1, slice_rows)
    spread = exchange(flipped, "section")
    picked = pick(section_to_group, spread)
    routed = exchange(picked, "section").reshape(shards, KVH, piece_cols, slice_rows)
    me = lax.axis_index("shard").astype(jnp.int32).reshape(1)
    received = exchange(pack(me, inputs, routed), "shard")
    base = KVH * slice_rows
    layer_out = received[:, :, :base].reshape(shards, piece_cols, KVH, slice_rows)
    layer_out = layer_out.transpose(2, 1, 0, 3).reshape(1, KVH, piece_cols, D)
    sums = jnp.sum(received[:, :, base:].astype(jnp.float32), axis=0)
    upper = jnp.concatenate([sums[:, : 2 * HD], sums[:, 2 * HD : 4 * HD]], axis=0)
    lower = jnp.concatenate([sums[:, 4 * HD : 5 * HD], sums[:, 5 * HD :]], axis=0)
    fresh = jnp.concatenate([upper[:, :HD] + lower, upper[:, HD:]], axis=1).astype(jnp.bfloat16)
    block_index = lax.axis_index("shard") % per_head
    row_lengths = lax.dynamic_slice_in_dim(lengths, block_index * row_block, row_block, 0)
    query_rows = queries.reshape(row_block, QPK, HD)
    context = attend(query_rows, kv_cache, fresh, row_lengths)
    return (context, layer_out)


def solution(mesh):
    return jax.shard_map(
        step,
        mesh=mesh,
        in_specs=(
            P("section", "shard", None),
            P(),
            P(("section", "shard"), None),
            P(("section", "shard"), None),
            P(("section", "shard"), None, None),
            P("section"),
        ),
        out_specs=(P(("section", "shard"), None), P("section", None, "shard", None)),
        check_vma=False,
    )
```

```python
import math

import jax
import jax.numpy as jnp
from jax import lax
from jax.experimental import pallas as pl
from jax.experimental.pallas import tpu as pltpu
from jax.sharding import PartitionSpec as P


D = 16384
HD = 128
QPK = 16
KVH = 4
LEN = 128
ROWS = 128


def exchange(blocks, axis):
    return lax.all_to_all(blocks, axis, split_axis=0, concat_axis=0, tiled=True)


def spread_rows(blocks):
    me = lax.axis_index("shard")
    shards = blocks.shape[0]

    def send(values, bits):
        return lax.ppermute(values, "shard", [(i, i ^ bits) for i in range(shards)])

    order = jnp.arange(shards, dtype=jnp.int32).reshape(4, 4, 2).transpose(2, 1, 0).reshape(-1)
    start = blocks.at[me ^ order].get(mode="promise_in_bounds")
    start = start.reshape((2, 4, 4) + blocks.shape[1:])
    side = [start[0], send(start[1], 1)]
    near = [jnp.stack([v[k] for v in side]) for k in range(4)]
    near = [near[0]] + [send(near[k], k << 1) for k in range(1, 4)]
    far = [jnp.stack([v[:, k] for v in near]) for k in range(4)]
    far = [far[0]] + [send(far[k], k << 3) for k in range(1, 4)]
    return jnp.concatenate(far).reshape((shards,) + blocks.shape[1:])


def attend(query_rows, cache_rows, fresh_rows, row_lengths):
    score_scale = 1.0 / math.sqrt(HD)
    cached_keys = cache_rows[:, :, :HD]
    cached_values = cache_rows[:, :, HD:]
    key_new = fresh_rows[:, :HD]
    value_new = fresh_rows[:, HD:]
    scores = (
        jnp.einsum("rhd,rtd->rht", query_rows, cached_keys, preferred_element_type=jnp.float32)
        * score_scale
    )
    valid = jnp.arange(LEN)[None, None, :] < row_lengths[:, None, None]
    scores = jnp.where(valid, scores, -1e30)
    fresh_score = (
        jnp.einsum("rhd,rd->rh", query_rows, key_new, preferred_element_type=jnp.float32)
        * score_scale
    )
    highest = jnp.maximum(jnp.max(scores, axis=-1), fresh_score)
    weights = jnp.where(valid, jnp.exp(scores - highest[..., None]), 0.0)
    fresh_weight = jnp.exp(fresh_score - highest)
    total = jnp.sum(weights, axis=-1) + fresh_weight
    probs = (weights / total[..., None]).astype(jnp.bfloat16)
    fresh_prob = (fresh_weight / total).astype(jnp.bfloat16)
    context = jnp.einsum("rht,rtd->rhd", probs, cached_values, preferred_element_type=jnp.float32)
    context = (
        context
        + fresh_prob.astype(jnp.float32)[..., None] * value_new.astype(jnp.float32)[:, None, :]
    )
    return context.reshape(context.shape[0], QPK * HD).astype(jnp.bfloat16)


VMEM = pl.BlockSpec(memory_space=pltpu.VMEM)


def flip_kernel(weights_ref, out_ref):
    step = pl.program_id(0)
    shards, heads, piece, _ = out_ref.shape
    rows = weights_ref.shape[1]
    lanes = pl.ds(pl.multiple_of(step * rows, rows), rows)
    for h in range(heads):
        width = shards * piece
        block = weights_ref[0, :, h * width : (h + 1) * width].astype(jnp.bfloat16)
        out_ref[:, h, :, lanes] = block.T.reshape(shards, piece, rows)


def flip(weights, shards):
    _, depth, columns = weights.shape
    piece = columns // KVH // shards
    rows = 128
    return pl.pallas_call(
        flip_kernel,
        grid=(depth // rows,),
        in_specs=[pl.BlockSpec((1, rows, columns), lambda i: (0, i, 0))],
        out_specs=VMEM,
        out_shape=jax.ShapeDtypeStruct((shards, KVH, piece, depth), jnp.bfloat16),
        cost_estimate=pl.CostEstimate(flops=2_000_000, bytes_accessed=3_000_000, transcendentals=0),
        compiler_params=pltpu.CompilerParams(vmem_limit_bytes=12 * 1024 * 1024),
        name="flip",
    )(weights)


def pick_kernel(group_ref, spread_ref, out_ref):
    def move(s, carry):
        out_ref[group_ref[s]] = spread_ref[s]
        return carry

    lax.fori_loop(0, spread_ref.shape[0], move, 0)


def pick(section_to_group, spread):
    return pl.pallas_call(
        pick_kernel,
        in_specs=[pl.BlockSpec(memory_space=pltpu.SMEM), VMEM],
        out_specs=VMEM,
        out_shape=jax.ShapeDtypeStruct(spread.shape, spread.dtype),
        cost_estimate=pl.CostEstimate(flops=1_000_000, bytes_accessed=2_000_000, transcendentals=0),
        compiler_params=pltpu.CompilerParams(vmem_limit_bytes=12 * 1024 * 1024),
        name="pick",
    )(section_to_group, spread)


def multiply_kernel(me_ref, inputs_ref, routed_ref, out_ref, rows_ref):
    me = me_ref[0]
    shards, heads, piece, depth = routed_ref.shape
    per_head = shards // heads
    own = inputs_ref.shape[1]
    block_rows = ROWS // per_head
    for d in range(shards):
        rows_ref[d * own : (d + 1) * own, :] = inputs_ref[me ^ d].astype(jnp.float32)
    inputs = rows_ref[...].astype(jnp.bfloat16)
    for h in range(heads):
        product = lax.dot_general(
            inputs,
            routed_ref[:, h].reshape(shards * piece, depth),
            (((1,), (1,)), ((), ())),
            preferred_element_type=jnp.float32,
        )
        for i in range(per_head):
            r = me ^ (h * per_head + i)
            out_ref[r & 1, (r >> 1) & 3, r >> 3] = product[i * block_rows : (i + 1) * block_rows]


def multiply(me, inputs, routed):
    shards, heads, _, depth = routed.shape
    return pl.pallas_call(
        multiply_kernel,
        in_specs=[pl.BlockSpec(memory_space=pltpu.SMEM), VMEM, VMEM],
        out_specs=VMEM,
        out_shape=jax.ShapeDtypeStruct((2, 4, 4, ROWS * heads // shards, 2 * HD), jnp.float32),
        scratch_shapes=[pltpu.VMEM((ROWS, depth), jnp.float32)],
        compiler_params=pltpu.CompilerParams(vmem_limit_bytes=12 * 1024 * 1024),
        cost_estimate=pl.CostEstimate(
            flops=2 * ROWS * heads * 2 * HD * depth, bytes_accessed=3_000_000, transcendentals=0
        ),
        name="multiply",
    )(me, inputs, routed)


def reduce_rows(partial):
    shards = lax.axis_size("shard")

    def send(values, bits):
        return lax.ppermute(values, "shard", [(i, i ^ bits) for i in range(shards)])

    partial = partial[0] + send(partial[1], 1)
    partial = partial[0] + (
        send(partial[1], 1 << 1) + (send(partial[2], 2 << 1) + send(partial[3], 3 << 1))
    )
    partial = partial[0] + (
        send(partial[1], 1 << 3) + (send(partial[2], 2 << 3) + send(partial[3], 3 << 3))
    )
    return partial


def step(train_weights, section_to_group, hidden, queries, kv_cache, lengths):
    shards = lax.axis_size("shard")
    sections = lax.axis_size("section")
    per_head = shards // KVH
    row_block = ROWS // per_head
    piece_cols = 2 * HD // shards
    slice_rows = train_weights.shape[1]
    own = hidden.shape[0]
    inputs = spread_rows(hidden.reshape(own, shards, slice_rows).transpose(1, 0, 2))
    flipped = flip(train_weights, shards).reshape(sections, -1, slice_rows)
    spread = exchange(flipped, "section")
    picked = pick(section_to_group, spread)
    routed = exchange(picked, "section").reshape(shards, KVH, piece_cols, slice_rows)
    me = lax.axis_index("shard").astype(jnp.int32).reshape(1)
    received = exchange(routed, "shard")
    layer_out = received.transpose(1, 2, 0, 3).reshape(1, KVH, piece_cols, D)
    fresh = reduce_rows(multiply(me, inputs, routed)).astype(jnp.bfloat16)
    block_index = lax.axis_index("shard") % per_head
    row_lengths = lax.dynamic_slice_in_dim(lengths, block_index * row_block, row_block, 0)
    query_rows = queries.reshape(row_block, QPK, HD)
    context = attend(query_rows, kv_cache, fresh, row_lengths)
    return (context, layer_out)


def solution(mesh):
    return jax.shard_map(
        step,
        mesh=mesh,
        in_specs=(
            P("section", "shard", None),
            P(),
            P(("section", "shard"), None),
            P(("section", "shard"), None),
            P(("section", "shard"), None, None),
            P("section"),
        ),
        out_specs=(P(("section", "shard"), None), P("section", None, "shard", None)),
        check_vma=False,
    )
```

```python
import math

import jax
import jax.numpy as jnp
from jax import lax
from jax.experimental import pallas as pl
from jax.experimental.pallas import tpu as pltpu
from jax.sharding import PartitionSpec as P


D = 16384
HD = 128
QPK = 16
KVH = 4
LEN = 128
ROWS = 128


def exchange(blocks, axis):
    return lax.all_to_all(blocks, axis, split_axis=0, concat_axis=0, tiled=True)


def spread_rows(blocks):
    me = lax.axis_index("shard")
    shards = blocks.shape[0]

    def send(values, bits):
        return lax.ppermute(values, "shard", [(i, i ^ bits) for i in range(shards)])

    order = jnp.arange(shards, dtype=jnp.int32).reshape(4, 4, 2).transpose(2, 1, 0).reshape(-1)
    start = blocks.at[me ^ order].get(mode="promise_in_bounds")
    start = start.reshape((2, 4, 4) + blocks.shape[1:])
    side = [start[0], send(start[1], 1)]
    near = [jnp.stack([v[k] for v in side]) for k in range(4)]
    near = [near[0]] + [send(near[k], k << 1) for k in range(1, 4)]
    far = [jnp.stack([v[:, k] for v in near]) for k in range(4)]
    far = [far[0]] + [send(far[k], k << 3) for k in range(1, 4)]
    return jnp.concatenate(far).reshape((shards,) + blocks.shape[1:])


def attend(query_rows, cache_rows, fresh_rows, row_lengths):
    score_scale = 1.0 / math.sqrt(HD)
    cached_keys = cache_rows[:, :, :HD]
    cached_values = cache_rows[:, :, HD:]
    key_new = fresh_rows[:, :HD]
    value_new = fresh_rows[:, HD:]
    scores = (
        jnp.einsum("rhd,rtd->rht", query_rows, cached_keys, preferred_element_type=jnp.float32)
        * score_scale
    )
    valid = jnp.arange(LEN)[None, None, :] < row_lengths[:, None, None]
    scores = jnp.where(valid, scores, -1e30)
    fresh_score = (
        jnp.einsum("rhd,rd->rh", query_rows, key_new, preferred_element_type=jnp.float32)
        * score_scale
    )
    highest = jnp.maximum(jnp.max(scores, axis=-1), fresh_score)
    weights = jnp.where(valid, jnp.exp(scores - highest[..., None]), 0.0)
    fresh_weight = jnp.exp(fresh_score - highest)
    total = jnp.sum(weights, axis=-1) + fresh_weight
    probs = (weights / total[..., None]).astype(jnp.bfloat16)
    fresh_prob = (fresh_weight / total).astype(jnp.bfloat16)
    context = jnp.einsum("rht,rtd->rhd", probs, cached_values, preferred_element_type=jnp.float32)
    context = (
        context
        + fresh_prob.astype(jnp.float32)[..., None] * value_new.astype(jnp.float32)[:, None, :]
    )
    return context.reshape(context.shape[0], QPK * HD).astype(jnp.bfloat16)


VMEM = pl.BlockSpec(memory_space=pltpu.VMEM)


def flip_kernel(weights_ref, out_ref):
    step = pl.program_id(0)
    shards, heads, piece, _ = out_ref.shape
    rows = weights_ref.shape[1]
    lanes = pl.ds(pl.multiple_of(step * rows, rows), rows)
    for h in range(heads):
        width = shards * piece
        block = weights_ref[0, :, h * width : (h + 1) * width].astype(jnp.bfloat16)
        out_ref[:, h, :, lanes] = block.T.reshape(shards, piece, rows)


def flip(weights, shards):
    _, depth, columns = weights.shape
    piece = columns // KVH // shards
    rows = 128
    return pl.pallas_call(
        flip_kernel,
        grid=(depth // rows,),
        in_specs=[pl.BlockSpec((1, rows, columns), lambda i: (0, i, 0))],
        out_specs=VMEM,
        out_shape=jax.ShapeDtypeStruct((shards, KVH, piece, depth), jnp.bfloat16),
        cost_estimate=pl.CostEstimate(flops=2_000_000, bytes_accessed=3_000_000, transcendentals=0),
        compiler_params=pltpu.CompilerParams(vmem_limit_bytes=12 * 1024 * 1024),
        name="flip",
    )(weights)


def pick_kernel(group_ref, spread_ref, out_ref):
    def move(s, carry):
        out_ref[group_ref[s]] = spread_ref[s]
        return carry

    lax.fori_loop(0, spread_ref.shape[0], move, 0)


def pick(section_to_group, spread):
    return pl.pallas_call(
        pick_kernel,
        in_specs=[pl.BlockSpec(memory_space=pltpu.SMEM), VMEM],
        out_specs=VMEM,
        out_shape=jax.ShapeDtypeStruct(spread.shape, spread.dtype),
        cost_estimate=pl.CostEstimate(flops=1_000_000, bytes_accessed=2_000_000, transcendentals=0),
        compiler_params=pltpu.CompilerParams(vmem_limit_bytes=12 * 1024 * 1024),
        name="pick",
    )(section_to_group, spread)


def multiply_kernel(me_ref, inputs_ref, routed_ref, out_ref, rows_ref):
    me = me_ref[0]
    shards, heads, piece, depth = routed_ref.shape
    per_head = shards // heads
    own = inputs_ref.shape[1]
    block_rows = ROWS // per_head
    for d in range(shards):
        rows_ref[d * own : (d + 1) * own, :] = inputs_ref[me ^ d].astype(jnp.float32)
    inputs = rows_ref[...].astype(jnp.bfloat16)
    for h in range(heads):
        product = lax.dot_general(
            inputs,
            routed_ref[:, h].reshape(shards * piece, depth),
            (((1,), (1,)), ((), ())),
            preferred_element_type=jnp.float32,
        )
        for i in range(per_head):
            r = me ^ (h * per_head + i)
            out_ref[r & 1, r >> 2, (r >> 1) & 1] = product[i * block_rows : (i + 1) * block_rows]


def multiply(me, inputs, routed):
    shards, heads, _, depth = routed.shape
    return pl.pallas_call(
        multiply_kernel,
        in_specs=[pl.BlockSpec(memory_space=pltpu.SMEM), VMEM, VMEM],
        out_specs=VMEM,
        out_shape=jax.ShapeDtypeStruct((2, 8, 2, ROWS * heads // shards, 2 * HD), jnp.float32),
        scratch_shapes=[pltpu.VMEM((ROWS, depth), jnp.float32)],
        compiler_params=pltpu.CompilerParams(vmem_limit_bytes=12 * 1024 * 1024),
        cost_estimate=pl.CostEstimate(
            flops=2 * ROWS * heads * 2 * HD * depth, bytes_accessed=3_000_000, transcendentals=0
        ),
        name="multiply",
    )(me, inputs, routed)


def reduce_rows(partial):
    shards = lax.axis_size("shard")

    def send(values, bits):
        return lax.ppermute(values, "shard", [(i, i ^ bits) for i in range(shards)])

    partial = partial[0] + send(partial[1], 1)
    arrived = [send(partial[k], k << 2) for k in range(1, 8)]
    partial = sum(arrived, partial[0])
    partial = partial[0] + send(partial[1], 1 << 1)
    return partial


def step(train_weights, section_to_group, hidden, queries, kv_cache, lengths):
    shards = lax.axis_size("shard")
    sections = lax.axis_size("section")
    per_head = shards // KVH
    row_block = ROWS // per_head
    piece_cols = 2 * HD // shards
    slice_rows = train_weights.shape[1]
    own = hidden.shape[0]
    inputs = spread_rows(hidden.reshape(own, shards, slice_rows).transpose(1, 0, 2))
    flipped = flip(train_weights, shards).reshape(sections, -1, slice_rows)
    spread = exchange(flipped, "section")
    picked = pick(section_to_group, spread)
    routed = exchange(picked, "section").reshape(shards, KVH, piece_cols, slice_rows)
    me = lax.axis_index("shard").astype(jnp.int32).reshape(1)
    received = exchange(routed, "shard")
    layer_out = received.transpose(1, 2, 0, 3).reshape(1, KVH, piece_cols, D)
    fresh = reduce_rows(multiply(me, inputs, routed)).astype(jnp.bfloat16)
    block_index = lax.axis_index("shard") % per_head
    row_lengths = lax.dynamic_slice_in_dim(lengths, block_index * row_block, row_block, 0)
    query_rows = queries.reshape(row_block, QPK, HD)
    context = attend(query_rows, kv_cache, fresh, row_lengths)
    return (context, layer_out)


def solution(mesh):
    return jax.shard_map(
        step,
        mesh=mesh,
        in_specs=(
            P("section", "shard", None),
            P(),
            P(("section", "shard"), None),
            P(("section", "shard"), None),
            P(("section", "shard"), None, None),
            P("section"),
        ),
        out_specs=(P(("section", "shard"), None), P("section", None, "shard", None)),
        check_vma=False,
    )
```

```python
import math

import jax
import jax.numpy as jnp
from jax import lax
from jax.experimental import pallas as pl
from jax.experimental.pallas import tpu as pltpu
from jax.sharding import PartitionSpec as P


D = 16384
HD = 128
QPK = 16
KVH = 4
LEN = 128
ROWS = 128


def exchange(blocks, axis):
    return lax.all_to_all(blocks, axis, split_axis=0, concat_axis=0, tiled=True)


def spread_rows(blocks):
    me = lax.axis_index("shard")
    shards = blocks.shape[0]

    def send(values, bits):
        return lax.ppermute(values, "shard", [(i, i ^ bits) for i in range(shards)])

    order = jnp.arange(shards, dtype=jnp.int32).reshape(4, 4, 2).transpose(2, 1, 0).reshape(-1)
    start = blocks.at[me ^ order].get(mode="promise_in_bounds")
    start = start.reshape((2, 4, 4) + blocks.shape[1:])
    side = [start[0], send(start[1], 1)]
    near = [jnp.stack([v[k] for v in side]) for k in range(4)]
    near = [near[0]] + [send(near[k], k << 1) for k in range(1, 4)]
    far = [jnp.stack([v[:, k] for v in near]) for k in range(4)]
    far = [far[0]] + [send(far[k], k << 3) for k in range(1, 4)]
    return jnp.concatenate(far).reshape((shards,) + blocks.shape[1:])


def attend(query_rows, cache_rows, fresh_rows, row_lengths):
    score_scale = 1.0 / math.sqrt(HD)
    cached_keys = cache_rows[:, :, :HD]
    cached_values = cache_rows[:, :, HD:]
    key_new = fresh_rows[:, :HD]
    value_new = fresh_rows[:, HD:]
    scores = (
        jnp.einsum("rhd,rtd->rht", query_rows, cached_keys, preferred_element_type=jnp.float32)
        * score_scale
    )
    valid = jnp.arange(LEN)[None, None, :] < row_lengths[:, None, None]
    scores = jnp.where(valid, scores, -1e30)
    fresh_score = (
        jnp.einsum("rhd,rd->rh", query_rows, key_new, preferred_element_type=jnp.float32)
        * score_scale
    )
    highest = jnp.maximum(jnp.max(scores, axis=-1), fresh_score)
    weights = jnp.where(valid, jnp.exp(scores - highest[..., None]), 0.0)
    fresh_weight = jnp.exp(fresh_score - highest)
    total = jnp.sum(weights, axis=-1) + fresh_weight
    probs = (weights / total[..., None]).astype(jnp.bfloat16)
    fresh_prob = (fresh_weight / total).astype(jnp.bfloat16)
    context = jnp.einsum("rht,rtd->rhd", probs, cached_values, preferred_element_type=jnp.float32)
    context = (
        context
        + fresh_prob.astype(jnp.float32)[..., None] * value_new.astype(jnp.float32)[:, None, :]
    )
    return context.reshape(context.shape[0], QPK * HD).astype(jnp.bfloat16)


VMEM = pl.BlockSpec(memory_space=pltpu.VMEM)


def flip_kernel(weights_ref, out_ref):
    step = pl.program_id(0)
    shards, piece, width = out_ref.shape
    rows = weights_ref.shape[1]
    for h in range(KVH):
        lanes = pl.ds(pl.multiple_of(h * (width // KVH) + step * rows, rows), rows)
        columns = shards * piece
        block = weights_ref[0, :, h * columns : (h + 1) * columns].astype(jnp.bfloat16)
        out_ref[:, :, lanes] = block.T.reshape(shards, piece, rows)


def flip(weights, shards):
    _, depth, columns = weights.shape
    piece = columns // KVH // shards
    rows = 128
    return pl.pallas_call(
        flip_kernel,
        grid=(depth // rows,),
        in_specs=[pl.BlockSpec((1, rows, columns), lambda i: (0, i, 0))],
        out_specs=VMEM,
        out_shape=jax.ShapeDtypeStruct((shards, piece, KVH * depth), jnp.bfloat16),
        cost_estimate=pl.CostEstimate(flops=2_000_000, bytes_accessed=3_000_000, transcendentals=0),
        compiler_params=pltpu.CompilerParams(vmem_limit_bytes=62 * 1024 * 1024),
        name="flip",
    )(weights)


def pick_kernel(group_ref, spread_ref, out_ref):
    def move(s, carry):
        out_ref[group_ref[s]] = spread_ref[s]
        return carry

    lax.fori_loop(0, spread_ref.shape[0], move, 0)


def pick(section_to_group, spread):
    return pl.pallas_call(
        pick_kernel,
        in_specs=[pl.BlockSpec(memory_space=pltpu.SMEM), VMEM],
        out_specs=VMEM,
        out_shape=jax.ShapeDtypeStruct(spread.shape, spread.dtype),
        cost_estimate=pl.CostEstimate(flops=1_000_000, bytes_accessed=2_000_000, transcendentals=0),
        compiler_params=pltpu.CompilerParams(vmem_limit_bytes=12 * 1024 * 1024),
        name="pick",
    )(section_to_group, spread)


def multiply_kernel(me_ref, inputs_ref, routed_ref, out_ref, rows_ref):
    me = me_ref[0]
    shards, piece, width = routed_ref.shape
    heads, depth = KVH, width // KVH
    per_head = shards // heads
    own = inputs_ref.shape[1]
    block_rows = ROWS // per_head
    for d in range(shards):
        rows_ref[d * own : (d + 1) * own, :] = inputs_ref[me ^ d].astype(jnp.float32)
    inputs = rows_ref[...].astype(jnp.bfloat16)
    for h in range(heads):
        product = lax.dot_general(
            inputs,
            routed_ref[:, :, h * depth : (h + 1) * depth].reshape(shards * piece, depth),
            (((1,), (1,)), ((), ())),
            preferred_element_type=jnp.float32,
        )
        for i in range(per_head):
            r = me ^ (h * per_head + i)
            out_ref[r & 1, r >> 2, (r >> 1) & 1] = product[i * block_rows : (i + 1) * block_rows]


def multiply(me, inputs, routed):
    shards, _, width = routed.shape
    heads, depth = KVH, width // KVH
    return pl.pallas_call(
        multiply_kernel,
        in_specs=[pl.BlockSpec(memory_space=pltpu.SMEM), VMEM, VMEM],
        out_specs=VMEM,
        out_shape=jax.ShapeDtypeStruct((2, 8, 2, ROWS * heads // shards, 2 * HD), jnp.float32),
        scratch_shapes=[pltpu.VMEM((ROWS, depth), jnp.float32)],
        compiler_params=pltpu.CompilerParams(vmem_limit_bytes=12 * 1024 * 1024),
        cost_estimate=pl.CostEstimate(
            flops=2 * ROWS * heads * 2 * HD * depth, bytes_accessed=3_000_000, transcendentals=0
        ),
        name="multiply",
    )(me, inputs, routed)


def reduce_rows(partial):
    shards = lax.axis_size("shard")

    def send(values, bits):
        return lax.ppermute(values, "shard", [(i, i ^ bits) for i in range(shards)])

    partial = partial[0] + send(partial[1], 1)
    arrived = [send(partial[k], k << 2) for k in range(1, 8)]
    partial = sum(arrived, partial[0])
    partial = partial[0] + send(partial[1], 1 << 1)
    return partial


def step(train_weights, section_to_group, hidden, queries, kv_cache, lengths):
    shards = lax.axis_size("shard")
    sections = lax.axis_size("section")
    per_head = shards // KVH
    row_block = ROWS // per_head
    piece_cols = 2 * HD // shards
    slice_rows = train_weights.shape[1]
    own = hidden.shape[0]
    inputs = spread_rows(hidden.reshape(own, shards, slice_rows).transpose(1, 0, 2))
    flipped = flip(train_weights, shards)
    flipped = flipped.reshape(sections, -1, KVH * slice_rows)
    spread = exchange(flipped, "section")
    picked = pick(section_to_group, spread)
    routed = exchange(picked, "section").reshape(shards, piece_cols, KVH * slice_rows)
    me = lax.axis_index("shard").astype(jnp.int32).reshape(1)
    received = exchange(routed, "shard")
    layer_out = received.reshape(shards, piece_cols, KVH, slice_rows)
    layer_out = layer_out.transpose(2, 1, 0, 3).reshape(1, KVH, piece_cols, D)
    fresh = reduce_rows(multiply(me, inputs, routed)).astype(jnp.bfloat16)
    block_index = lax.axis_index("shard") % per_head
    row_lengths = lax.dynamic_slice_in_dim(lengths, block_index * row_block, row_block, 0)
    query_rows = queries.reshape(row_block, QPK, HD)
    context = attend(query_rows, kv_cache, fresh, row_lengths)
    return (context, layer_out)


def solution(mesh):
    return jax.shard_map(
        step,
        mesh=mesh,
        in_specs=(
            P("section", "shard", None),
            P(),
            P(("section", "shard"), None),
            P(("section", "shard"), None),
            P(("section", "shard"), None, None),
            P("section"),
        ),
        out_specs=(P(("section", "shard"), None), P("section", None, "shard", None)),
        check_vma=False,
    )
```

```python
import math

import jax
import jax.numpy as jnp
from jax import lax
from jax.experimental import pallas as pl
from jax.experimental.pallas import tpu as pltpu
from jax.sharding import PartitionSpec as P


D = 16384
HD = 128
QPK = 16
KVH = 4
LEN = 128
ROWS = 128


def exchange(blocks, axis):
    return lax.all_to_all(blocks, axis, split_axis=0, concat_axis=0, tiled=True)


def spread_rows(blocks):
    me = lax.axis_index("shard")
    shards = blocks.shape[0]

    def send(values, bits):
        return lax.ppermute(values, "shard", [(i, i ^ bits) for i in range(shards)])

    order = jnp.arange(shards, dtype=jnp.int32).reshape(4, 4, 2).transpose(2, 1, 0).reshape(-1)
    start = blocks.at[me ^ order].get(mode="promise_in_bounds")
    start = start.reshape((2, 4, 4) + blocks.shape[1:])
    side = [start[0], send(start[1], 1)]
    near = [jnp.stack([v[k] for v in side]) for k in range(4)]
    near = [near[0]] + [send(near[k], k << 1) for k in range(1, 4)]
    far = [jnp.stack([v[:, k] for v in near]) for k in range(4)]
    for k in (2, 1, 3):
        far[k] = send(far[k], k << 3)
    return jnp.concatenate(far).reshape((shards,) + blocks.shape[1:])


def attend(query_rows, cache_rows, fresh_rows, row_lengths):
    score_scale = 1.0 / math.sqrt(HD)
    cached_keys = cache_rows[:, :, :HD]
    cached_values = cache_rows[:, :, HD:]
    key_new = fresh_rows[:, :HD]
    value_new = fresh_rows[:, HD:]
    scores = (
        jnp.einsum("rhd,rtd->rht", query_rows, cached_keys, preferred_element_type=jnp.float32)
        * score_scale
    )
    valid = jnp.arange(LEN)[None, None, :] < row_lengths[:, None, None]
    scores = jnp.where(valid, scores, -1e30)
    fresh_score = (
        jnp.einsum("rhd,rd->rh", query_rows, key_new, preferred_element_type=jnp.float32)
        * score_scale
    )
    highest = jnp.maximum(jnp.max(scores, axis=-1), fresh_score)
    weights = jnp.where(valid, jnp.exp(scores - highest[..., None]), 0.0)
    fresh_weight = jnp.exp(fresh_score - highest)
    total = jnp.sum(weights, axis=-1) + fresh_weight
    probs = (weights / total[..., None]).astype(jnp.bfloat16)
    fresh_prob = (fresh_weight / total).astype(jnp.bfloat16)
    context = jnp.einsum("rht,rtd->rhd", probs, cached_values, preferred_element_type=jnp.float32)
    context = (
        context
        + fresh_prob.astype(jnp.float32)[..., None] * value_new.astype(jnp.float32)[:, None, :]
    )
    return context.reshape(context.shape[0], QPK * HD).astype(jnp.bfloat16)


VMEM = pl.BlockSpec(memory_space=pltpu.VMEM)


def flip_kernel(weights_ref, out_ref):
    step = pl.program_id(0)
    shards, piece, width = out_ref.shape
    rows = weights_ref.shape[1]
    for h in range(KVH):
        lanes = pl.ds(pl.multiple_of(h * (width // KVH) + step * rows, rows), rows)
        columns = shards * piece
        block = weights_ref[0, :, h * columns : (h + 1) * columns].astype(jnp.bfloat16)
        out_ref[:, :, lanes] = block.T.reshape(shards, piece, rows)


def flip(weights, shards):
    _, depth, columns = weights.shape
    piece = columns // KVH // shards
    rows = 128
    return pl.pallas_call(
        flip_kernel,
        grid=(depth // rows,),
        in_specs=[pl.BlockSpec((1, rows, columns), lambda i: (0, i, 0))],
        out_specs=VMEM,
        out_shape=jax.ShapeDtypeStruct((shards, piece, KVH * depth), jnp.bfloat16),
        cost_estimate=pl.CostEstimate(flops=2_000_000, bytes_accessed=3_000_000, transcendentals=0),
        compiler_params=pltpu.CompilerParams(vmem_limit_bytes=62 * 1024 * 1024),
        name="flip",
    )(weights)


def pick_kernel(group_ref, spread_ref, out_ref):
    def move(s, carry):
        out_ref[group_ref[s]] = spread_ref[s]
        return carry

    lax.fori_loop(0, spread_ref.shape[0], move, 0)


def pick(section_to_group, spread):
    return pl.pallas_call(
        pick_kernel,
        in_specs=[pl.BlockSpec(memory_space=pltpu.SMEM), VMEM],
        out_specs=VMEM,
        out_shape=jax.ShapeDtypeStruct(spread.shape, spread.dtype),
        cost_estimate=pl.CostEstimate(flops=1_000_000, bytes_accessed=2_000_000, transcendentals=0),
        compiler_params=pltpu.CompilerParams(vmem_limit_bytes=12 * 1024 * 1024),
        name="pick",
    )(section_to_group, spread)


def multiply_kernel(me_ref, inputs_ref, routed_ref, out_ref, rows_ref):
    me = me_ref[0]
    shards, piece, width = routed_ref.shape
    heads, depth = KVH, width // KVH
    per_head = shards // heads
    own = inputs_ref.shape[1]
    block_rows = ROWS // per_head
    for d in range(shards):
        rows_ref[d * own : (d + 1) * own, :] = inputs_ref[me ^ d].astype(jnp.float32)
    inputs = rows_ref[...].astype(jnp.bfloat16)
    for h in range(heads):
        product = lax.dot_general(
            inputs,
            routed_ref[:, :, h * depth : (h + 1) * depth].reshape(shards * piece, depth),
            (((1,), (1,)), ((), ())),
            preferred_element_type=jnp.float32,
        )
        for i in range(per_head):
            r = me ^ (h * per_head + i)
            out_ref[r & 1, r >> 2, (r >> 1) & 1] = product[i * block_rows : (i + 1) * block_rows]


def multiply(me, inputs, routed):
    shards, _, width = routed.shape
    heads, depth = KVH, width // KVH
    return pl.pallas_call(
        multiply_kernel,
        in_specs=[pl.BlockSpec(memory_space=pltpu.SMEM), VMEM, VMEM],
        out_specs=VMEM,
        out_shape=jax.ShapeDtypeStruct((2, 8, 2, ROWS * heads // shards, 2 * HD), jnp.float32),
        scratch_shapes=[pltpu.VMEM((ROWS, depth), jnp.float32)],
        compiler_params=pltpu.CompilerParams(vmem_limit_bytes=12 * 1024 * 1024),
        cost_estimate=pl.CostEstimate(
            flops=2 * ROWS * heads * 2 * HD * depth, bytes_accessed=3_000_000, transcendentals=0
        ),
        name="multiply",
    )(me, inputs, routed)


def reduce_rows(partial):
    shards = lax.axis_size("shard")

    def send(values, bits):
        return lax.ppermute(values, "shard", [(i, i ^ bits) for i in range(shards)])

    partial = partial[0] + send(partial[1], 1)
    head = lax.reduce_precision(partial[1:], 8, 7)
    rest = partial[1:, :, :, :HD] - head[:, :, :, :HD]
    halves = jnp.concatenate([head, rest], axis=-1).astype(jnp.bfloat16)
    arrived = {}
    for k in (4, 5, 3, 6, 2, 7, 1):
        arrived[k] = send(halves[k - 1], k << 2)
    total = sum(v.astype(jnp.float32) for v in arrived.values())
    keys = total[:, :, :HD] + total[:, :, 2 * HD :]
    partial = partial[0] + jnp.concatenate([keys, total[:, :, HD : 2 * HD]], axis=-1)
    partial = partial[0] + send(partial[1], 1 << 1)
    return partial


def step(train_weights, section_to_group, hidden, queries, kv_cache, lengths):
    shards = lax.axis_size("shard")
    sections = lax.axis_size("section")
    per_head = shards // KVH
    row_block = ROWS // per_head
    piece_cols = 2 * HD // shards
    slice_rows = train_weights.shape[1]
    own = hidden.shape[0]
    inputs = spread_rows(hidden.reshape(own, shards, slice_rows).transpose(1, 0, 2))
    flipped = flip(train_weights, shards)
    flipped = flipped.reshape(sections, -1, KVH * slice_rows)
    spread = exchange(flipped, "section")
    picked = pick(section_to_group, spread)
    routed = exchange(picked, "section").reshape(shards, piece_cols, KVH * slice_rows)
    me = lax.axis_index("shard").astype(jnp.int32).reshape(1)
    received = exchange(routed, "shard")
    layer_out = received.reshape(shards, piece_cols, KVH, slice_rows)
    layer_out = layer_out.transpose(2, 1, 0, 3).reshape(1, KVH, piece_cols, D)
    fresh = reduce_rows(multiply(me, inputs, routed)).astype(jnp.bfloat16)
    block_index = lax.axis_index("shard") % per_head
    row_lengths = lax.dynamic_slice_in_dim(lengths, block_index * row_block, row_block, 0)
    query_rows = queries.reshape(row_block, QPK, HD)
    context = attend(query_rows, kv_cache, fresh, row_lengths)
    return (context, layer_out)


def solution(mesh):
    return jax.shard_map(
        step,
        mesh=mesh,
        in_specs=(
            P("section", "shard", None),
            P(),
            P(("section", "shard"), None),
            P(("section", "shard"), None),
            P(("section", "shard"), None, None),
            P("section"),
        ),
        out_specs=(P(("section", "shard"), None), P("section", None, "shard", None)),
        check_vma=False,
    )
```

```python
import math

import jax
import jax.numpy as jnp
from jax import lax
from jax.experimental import pallas as pl
from jax.experimental.pallas import tpu as pltpu
from jax.sharding import PartitionSpec as P


D = 16384
HD = 128
QPK = 16
KVH = 4
LEN = 128
ROWS = 128
ROW_TILE = 128


def exchange(blocks, axis):
    return lax.all_to_all(blocks, axis, split_axis=0, concat_axis=0, tiled=True)


def spread_rows(blocks):
    me = lax.axis_index("shard")
    shards = blocks.shape[0]

    def send(values, bits):
        return lax.ppermute(values, "shard", [(i, i ^ bits) for i in range(shards)])

    order = jnp.arange(shards, dtype=jnp.int32).reshape(4, 4, 2).transpose(2, 1, 0).reshape(-1)
    start = blocks.at[me ^ order].get(mode="promise_in_bounds")
    start = start.reshape((2, 4, 4) + blocks.shape[1:])
    side = [start[0], send(start[1], 1)]
    near = [jnp.stack([v[k] for v in side]) for k in range(4)]
    near = [near[0]] + [send(near[k], k << 1) for k in range(1, 4)]
    far = [jnp.stack([v[:, k] for v in near]) for k in range(4)]
    for k in (2, 1, 3):
        far[k] = send(far[k], k << 3)
    return jnp.concatenate(far).reshape((shards,) + blocks.shape[1:])


def attend(query_rows, cache_rows, fresh_rows, row_lengths):
    score_scale = 1.0 / math.sqrt(HD)
    cached_keys = cache_rows[:, :, :HD]
    cached_values = cache_rows[:, :, HD:]
    key_new = fresh_rows[:, :HD]
    value_new = fresh_rows[:, HD:]
    scores = (
        jnp.einsum("rhd,rtd->rht", query_rows, cached_keys, preferred_element_type=jnp.float32)
        * score_scale
    )
    valid = jnp.arange(LEN)[None, None, :] < row_lengths[:, None, None]
    scores = jnp.where(valid, scores, -1e30)
    fresh_score = (
        jnp.einsum("rhd,rd->rh", query_rows, key_new, preferred_element_type=jnp.float32)
        * score_scale
    )
    highest = jnp.maximum(jnp.max(scores, axis=-1), fresh_score)
    weights = jnp.where(valid, jnp.exp(scores - highest[..., None]), 0.0)
    fresh_weight = jnp.exp(fresh_score - highest)
    total = jnp.sum(weights, axis=-1) + fresh_weight
    probs = (weights / total[..., None]).astype(jnp.bfloat16)
    fresh_prob = (fresh_weight / total).astype(jnp.bfloat16)
    context = jnp.einsum("rht,rtd->rhd", probs, cached_values, preferred_element_type=jnp.float32)
    context = (
        context
        + fresh_prob.astype(jnp.float32)[..., None] * value_new.astype(jnp.float32)[:, None, :]
    )
    return context.reshape(context.shape[0], QPK * HD).astype(jnp.bfloat16)


VMEM = pl.BlockSpec(memory_space=pltpu.VMEM)


def flip_kernel(weights_ref, out_ref):
    shards, piece, width = out_ref.shape
    rows = width // KVH
    columns = shards * piece
    for h in range(KVH):
        block = weights_ref[0, :, h * columns : (h + 1) * columns].astype(jnp.bfloat16)
        out_ref[:, :, h * rows : (h + 1) * rows] = block.T.reshape(shards, piece, rows)


def flip(weights, shards):
    _, depth, columns = weights.shape
    piece = columns // KVH // shards
    return pl.pallas_call(
        flip_kernel,
        grid=(depth // ROW_TILE,),
        in_specs=[pl.BlockSpec((1, ROW_TILE, columns), lambda i: (0, i, 0))],
        out_specs=pl.BlockSpec((shards, piece, KVH * ROW_TILE), lambda i: (0, 0, i)),
        out_shape=jax.ShapeDtypeStruct((shards, piece, KVH * depth), jnp.bfloat16),
        cost_estimate=pl.CostEstimate(flops=2_000_000, bytes_accessed=3_000_000, transcendentals=0),
        compiler_params=pltpu.CompilerParams(vmem_limit_bytes=62 * 1024 * 1024),
        name="flip",
    )(weights)


def pick_kernel(group_ref, spread_ref, out_ref, sems):
    copies = [
        pltpu.make_async_copy(spread_ref.at[s], out_ref.at[group_ref[s]], sems.at[s])
        for s in range(spread_ref.shape[0])
    ]
    for copy in copies:
        copy.start()
    for copy in copies:
        copy.wait()


def pick(section_to_group, spread):
    return pl.pallas_call(
        pick_kernel,
        in_specs=[pl.BlockSpec(memory_space=pltpu.SMEM), VMEM],
        out_specs=pl.BlockSpec(memory_space=pltpu.HBM),
        out_shape=jax.ShapeDtypeStruct(spread.shape, spread.dtype),
        scratch_shapes=[pltpu.SemaphoreType.DMA((spread.shape[0],))],
        compiler_params=pltpu.CompilerParams(vmem_limit_bytes=12 * 1024 * 1024),
        cost_estimate=pl.CostEstimate(flops=1_000_000, bytes_accessed=2_000_000, transcendentals=0),
        name="pick",
    )(section_to_group, spread)


def multiply_kernel(me_ref, inputs_ref, routed_ref, out_ref, rows_ref):
    me = me_ref[0]
    shards, piece, width = routed_ref.shape
    heads, depth = KVH, width // KVH
    per_head = shards // heads
    own = inputs_ref.shape[1]
    block_rows = ROWS // per_head
    for d in range(shards):
        rows_ref[d * own : (d + 1) * own, :] = inputs_ref[me ^ d].astype(jnp.float32)
    inputs = rows_ref[...].astype(jnp.bfloat16)
    for h in range(heads):
        tiles = [
            routed_ref[:, :, (i * heads + h) * ROW_TILE : (i * heads + h + 1) * ROW_TILE]
            for i in range(depth // ROW_TILE)
        ]
        product = lax.dot_general(
            inputs,
            jnp.concatenate(tiles, axis=-1).reshape(shards * piece, depth),
            (((1,), (1,)), ((), ())),
            preferred_element_type=jnp.float32,
        )
        for i in range(per_head):
            r = me ^ (h * per_head + i)
            out_ref[r & 1, r >> 2, (r >> 1) & 1] = product[i * block_rows : (i + 1) * block_rows]


def multiply(me, inputs, routed):
    shards, _, width = routed.shape
    heads, depth = KVH, width // KVH
    return pl.pallas_call(
        multiply_kernel,
        in_specs=[pl.BlockSpec(memory_space=pltpu.SMEM), VMEM, VMEM],
        out_specs=VMEM,
        out_shape=jax.ShapeDtypeStruct((2, 8, 2, ROWS * heads // shards, 2 * HD), jnp.float32),
        scratch_shapes=[pltpu.VMEM((ROWS, depth), jnp.float32)],
        compiler_params=pltpu.CompilerParams(vmem_limit_bytes=12 * 1024 * 1024),
        cost_estimate=pl.CostEstimate(
            flops=2 * ROWS * heads * 2 * HD * depth, bytes_accessed=3_000_000, transcendentals=0
        ),
        name="multiply",
    )(me, inputs, routed)


def reduce_rows(partial):
    shards = lax.axis_size("shard")

    def send(values, bits):
        return lax.ppermute(values, "shard", [(i, i ^ bits) for i in range(shards)])

    partial = partial[0] + send(partial[1], 1)
    head = lax.reduce_precision(partial[1:], 8, 7)
    rest = partial[1:, :, :, :HD] - head[:, :, :, :HD]
    halves = jnp.concatenate([head, rest], axis=-1).astype(jnp.bfloat16)
    arrived = {}
    for k in (4, 5, 3, 6, 2, 7, 1):
        arrived[k] = send(halves[k - 1], k << 2)
    total = sum(v.astype(jnp.float32) for v in arrived.values())
    keys = total[:, :, :HD] + total[:, :, 2 * HD :]
    partial = partial[0] + jnp.concatenate([keys, total[:, :, HD : 2 * HD]], axis=-1)
    partial = partial[0] + send(partial[1], 1 << 1)
    return partial


def step(train_weights, section_to_group, hidden, queries, kv_cache, lengths):
    shards = lax.axis_size("shard")
    sections = lax.axis_size("section")
    per_head = shards // KVH
    row_block = ROWS // per_head
    piece_cols = 2 * HD // shards
    slice_rows = train_weights.shape[1]
    own = hidden.shape[0]
    inputs = spread_rows(hidden.reshape(own, shards, slice_rows).transpose(1, 0, 2))
    flipped = flip(train_weights, shards)
    flipped = flipped.reshape(sections, -1, KVH * slice_rows)
    spread = exchange(flipped, "section")
    picked = pick(section_to_group, spread)
    routed = exchange(picked, "section").reshape(shards, piece_cols, KVH * slice_rows)
    me = lax.axis_index("shard").astype(jnp.int32).reshape(1)
    received = exchange(routed, "shard")
    layer_out = received.reshape(shards, piece_cols, -1, KVH, ROW_TILE)
    layer_out = layer_out.transpose(3, 1, 0, 2, 4).reshape(1, KVH, piece_cols, D)
    fresh = reduce_rows(multiply(me, inputs, routed)).astype(jnp.bfloat16)
    block_index = lax.axis_index("shard") % per_head
    row_lengths = lax.dynamic_slice_in_dim(lengths, block_index * row_block, row_block, 0)
    query_rows = queries.reshape(row_block, QPK, HD)
    context = attend(query_rows, kv_cache, fresh, row_lengths)
    return (context, layer_out)


def solution(mesh):
    return jax.shard_map(
        step,
        mesh=mesh,
        in_specs=(
            P("section", "shard", None),
            P(),
            P(("section", "shard"), None),
            P(("section", "shard"), None),
            P(("section", "shard"), None, None),
            P("section"),
        ),
        out_specs=(P(("section", "shard"), None), P("section", None, "shard", None)),
        check_vma=False,
    )
```

```python
import math

import jax
import jax.numpy as jnp
from jax import lax
from jax.experimental import pallas as pl
from jax.experimental.pallas import tpu as pltpu
from jax.sharding import PartitionSpec as P


D = 16384
HD = 128
QPK = 16
KVH = 4
LEN = 128
ROWS = 128


def exchange(blocks, axis):
    return lax.all_to_all(blocks, axis, split_axis=0, concat_axis=0, tiled=True)


def spread_rows(blocks):
    me = lax.axis_index("shard")
    shards = blocks.shape[0]

    def send(values, bits):
        return lax.ppermute(values, "shard", [(i, i ^ bits) for i in range(shards)])

    order = jnp.arange(shards, dtype=jnp.int32).reshape(4, 4, 2).transpose(2, 0, 1).reshape(-1)
    start = blocks.at[me ^ order].get(mode="promise_in_bounds")
    start = start.reshape((2, 4, 4) + blocks.shape[1:])
    side = [start[0], send(start[1], 1)]
    far = [jnp.stack([v[k] for v in side]) for k in range(4)]
    for k in (2, 1, 3):
        far[k] = send(far[k], k << 3)
    near = [jnp.stack([v[:, k] for v in far]) for k in range(4)]
    near = [near[0]] + [send(near[k], k << 1) for k in range(1, 4)]
    return jnp.concatenate(near).reshape((shards,) + blocks.shape[1:])


def attend(query_rows, cache_rows, fresh_rows, row_lengths):
    score_scale = 1.0 / math.sqrt(HD)
    cached_keys = cache_rows[:, :, :HD]
    cached_values = cache_rows[:, :, HD:]
    key_new = fresh_rows[:, :HD]
    value_new = fresh_rows[:, HD:]
    scores = (
        jnp.einsum("rhd,rtd->rht", query_rows, cached_keys, preferred_element_type=jnp.float32)
        * score_scale
    )
    valid = jnp.arange(LEN)[None, None, :] < row_lengths[:, None, None]
    scores = jnp.where(valid, scores, -1e30)
    fresh_score = (
        jnp.einsum("rhd,rd->rh", query_rows, key_new, preferred_element_type=jnp.float32)
        * score_scale
    )
    highest = jnp.maximum(jnp.max(scores, axis=-1), fresh_score)
    weights = jnp.where(valid, jnp.exp(scores - highest[..., None]), 0.0)
    fresh_weight = jnp.exp(fresh_score - highest)
    total = jnp.sum(weights, axis=-1) + fresh_weight
    probs = (weights / total[..., None]).astype(jnp.bfloat16)
    fresh_prob = (fresh_weight / total).astype(jnp.bfloat16)
    context = jnp.einsum("rht,rtd->rhd", probs, cached_values, preferred_element_type=jnp.float32)
    context = (
        context
        + fresh_prob.astype(jnp.float32)[..., None] * value_new.astype(jnp.float32)[:, None, :]
    )
    return context.reshape(context.shape[0], QPK * HD).astype(jnp.bfloat16)


VMEM = pl.BlockSpec(memory_space=pltpu.VMEM)


def flip_kernel(weights_ref, out_ref):
    step = pl.program_id(0)
    shards, piece, width = out_ref.shape
    rows = weights_ref.shape[1]
    for h in range(KVH):
        lanes = pl.ds(pl.multiple_of(h * (width // KVH) + step * rows, rows), rows)
        columns = shards * piece
        block = weights_ref[0, :, h * columns : (h + 1) * columns].astype(jnp.bfloat16)
        out_ref[:, :, lanes] = block.T.reshape(shards, piece, rows)


def flip(weights, shards):
    _, depth, columns = weights.shape
    piece = columns // KVH // shards
    rows = 128
    return pl.pallas_call(
        flip_kernel,
        grid=(depth // rows,),
        in_specs=[pl.BlockSpec((1, rows, columns), lambda i: (0, i, 0))],
        out_specs=VMEM,
        out_shape=jax.ShapeDtypeStruct((shards, piece, KVH * depth), jnp.bfloat16),
        cost_estimate=pl.CostEstimate(flops=2_000_000, bytes_accessed=3_000_000, transcendentals=0),
        compiler_params=pltpu.CompilerParams(vmem_limit_bytes=62 * 1024 * 1024),
        name="flip",
    )(weights)


def pick_kernel(group_ref, spread_ref, out_ref):
    def move(s, carry):
        out_ref[group_ref[s]] = spread_ref[s]
        return carry

    lax.fori_loop(0, spread_ref.shape[0], move, 0)


def pick(section_to_group, spread):
    return pl.pallas_call(
        pick_kernel,
        in_specs=[pl.BlockSpec(memory_space=pltpu.SMEM), VMEM],
        out_specs=VMEM,
        out_shape=jax.ShapeDtypeStruct(spread.shape, spread.dtype),
        cost_estimate=pl.CostEstimate(flops=1_000_000, bytes_accessed=2_000_000, transcendentals=0),
        compiler_params=pltpu.CompilerParams(vmem_limit_bytes=12 * 1024 * 1024),
        name="pick",
    )(section_to_group, spread)


def multiply_kernel(me_ref, inputs_ref, routed_ref, out_ref, rows_ref):
    me = me_ref[0]
    shards, piece, width = routed_ref.shape
    heads, depth = KVH, width // KVH
    per_head = shards // heads
    own = inputs_ref.shape[1]
    block_rows = ROWS // per_head
    for d in range(shards):
        r = me ^ d
        place = ((r >> 1) & 3) * (shards // 4) + (r >> 3) * 2 + (r & 1)
        rows_ref[d * own : (d + 1) * own, :] = inputs_ref[place].astype(jnp.float32)
    inputs = rows_ref[...].astype(jnp.bfloat16)
    for h in range(heads):
        product = lax.dot_general(
            inputs,
            routed_ref[:, :, h * depth : (h + 1) * depth].reshape(shards * piece, depth),
            (((1,), (1,)), ((), ())),
            preferred_element_type=jnp.float32,
        )
        for i in range(per_head):
            r = me ^ (h * per_head + i)
            out_ref[r & 1, r >> 2, (r >> 1) & 1] = product[i * block_rows : (i + 1) * block_rows]


def multiply(me, inputs, routed):
    shards, _, width = routed.shape
    heads, depth = KVH, width // KVH
    return pl.pallas_call(
        multiply_kernel,
        in_specs=[pl.BlockSpec(memory_space=pltpu.SMEM), VMEM, VMEM],
        out_specs=VMEM,
        out_shape=jax.ShapeDtypeStruct((2, 8, 2, ROWS * heads // shards, 2 * HD), jnp.float32),
        scratch_shapes=[pltpu.VMEM((ROWS, depth), jnp.float32)],
        compiler_params=pltpu.CompilerParams(vmem_limit_bytes=12 * 1024 * 1024),
        cost_estimate=pl.CostEstimate(
            flops=2 * ROWS * heads * 2 * HD * depth, bytes_accessed=3_000_000, transcendentals=0
        ),
        name="multiply",
    )(me, inputs, routed)


def reduce_rows(partial):
    shards = lax.axis_size("shard")

    def send(values, bits):
        return lax.ppermute(values, "shard", [(i, i ^ bits) for i in range(shards)])

    partial = partial[0] + send(partial[1], 1)
    head = lax.reduce_precision(partial[1:], 8, 7)
    rest = partial[1:, :, :, :HD] - head[:, :, :, :HD]
    halves = jnp.concatenate([head, rest], axis=-1).astype(jnp.bfloat16)
    arrived = {}
    for k in (4, 5, 3, 6, 2, 7, 1):
        arrived[k] = send(halves[k - 1], k << 2)
    total = sum(v.astype(jnp.float32) for v in arrived.values())
    keys = total[:, :, :HD] + total[:, :, 2 * HD :]
    partial = partial[0] + jnp.concatenate([keys, total[:, :, HD : 2 * HD]], axis=-1)
    partial = partial[0] + send(partial[1], 1 << 1)
    return partial


def step(train_weights, section_to_group, hidden, queries, kv_cache, lengths):
    shards = lax.axis_size("shard")
    sections = lax.axis_size("section")
    per_head = shards // KVH
    row_block = ROWS // per_head
    piece_cols = 2 * HD // shards
    slice_rows = train_weights.shape[1]
    own = hidden.shape[0]
    inputs = spread_rows(hidden.reshape(own, shards, slice_rows).transpose(1, 0, 2))
    flipped = flip(train_weights, shards)
    flipped = flipped.reshape(sections, -1, KVH * slice_rows)
    spread = exchange(flipped, "section")
    picked = pick(section_to_group, spread)
    routed = exchange(picked, "section").reshape(shards, piece_cols, KVH * slice_rows)
    me = lax.axis_index("shard").astype(jnp.int32).reshape(1)
    received = exchange(routed, "shard")
    layer_out = received.reshape(shards, piece_cols, KVH, slice_rows)
    layer_out = layer_out.transpose(2, 1, 0, 3).reshape(1, KVH, piece_cols, D)
    fresh = reduce_rows(multiply(me, inputs, routed)).astype(jnp.bfloat16)
    block_index = lax.axis_index("shard") % per_head
    row_lengths = lax.dynamic_slice_in_dim(lengths, block_index * row_block, row_block, 0)
    query_rows = queries.reshape(row_block, QPK, HD)
    context = attend(query_rows, kv_cache, fresh, row_lengths)
    return (context, layer_out)


def solution(mesh):
    return jax.shard_map(
        step,
        mesh=mesh,
        in_specs=(
            P("section", "shard", None),
            P(),
            P(("section", "shard"), None),
            P(("section", "shard"), None),
            P(("section", "shard"), None, None),
            P("section"),
        ),
        out_specs=(P(("section", "shard"), None), P("section", None, "shard", None)),
        check_vma=False,
    )
```

```python
import math

import jax
import jax.numpy as jnp
from jax import lax
from jax.experimental import pallas as pl
from jax.experimental.pallas import tpu as pltpu
from jax.sharding import PartitionSpec as P


D = 16384
HD = 128
QPK = 16
KVH = 4
LEN = 128
ROWS = 128
ROW_TILE = 128


def exchange(blocks, axis):
    return lax.all_to_all(blocks, axis, split_axis=0, concat_axis=0, tiled=True)


def spread_rows(keep, other):
    shards = lax.axis_size("shard")

    def send(values, bits):
        return lax.ppermute(values, "shard", [(i, i ^ bits) for i in range(shards)])

    side = [keep, send(other, 1)]
    near = [jnp.stack([v[k] for v in side]) for k in range(4)]
    near = [near[0]] + [send(near[k], k << 1) for k in range(1, 4)]
    far = [jnp.stack([v[:, k] for v in near]) for k in range(4)]
    for k in (2, 1, 3):
        far[k] = send(far[k], k << 3)
    return jnp.concatenate(far).reshape((shards,) + keep.shape[2:])


def attend(query_rows, cache_rows, fresh_rows, row_lengths):
    score_scale = 1.0 / math.sqrt(HD)
    cached_keys = cache_rows[:, :, :HD]
    cached_values = cache_rows[:, :, HD:]
    key_new = fresh_rows[:, :HD]
    value_new = fresh_rows[:, HD:]
    scores = (
        jnp.einsum("rhd,rtd->rht", query_rows, cached_keys, preferred_element_type=jnp.float32)
        * score_scale
    )
    valid = jnp.arange(LEN)[None, None, :] < row_lengths[:, None, None]
    scores = jnp.where(valid, scores, -1e30)
    fresh_score = (
        jnp.einsum("rhd,rd->rh", query_rows, key_new, preferred_element_type=jnp.float32)
        * score_scale
    )
    highest = jnp.maximum(jnp.max(scores, axis=-1), fresh_score)
    weights = jnp.where(valid, jnp.exp(scores - highest[..., None]), 0.0)
    fresh_weight = jnp.exp(fresh_score - highest)
    total = jnp.sum(weights, axis=-1) + fresh_weight
    probs = (weights / total[..., None]).astype(jnp.bfloat16)
    fresh_prob = (fresh_weight / total).astype(jnp.bfloat16)
    context = jnp.einsum("rht,rtd->rhd", probs, cached_values, preferred_element_type=jnp.float32)
    context = (
        context
        + fresh_prob.astype(jnp.float32)[..., None] * value_new.astype(jnp.float32)[:, None, :]
    )
    return context.reshape(context.shape[0], QPK * HD).astype(jnp.bfloat16)


VMEM = pl.BlockSpec(memory_space=pltpu.VMEM)


def enter_kernel(
    me_ref, weights_ref, hidden_ref, out_ref, keep_ref, send_ref,
    weights_buf, out_buf, hidden_buf, in_sems, out_sems, hidden_sem,
):
    steps, rows, _ = weights_buf.shape
    _, shards, piece, width = out_buf.shape
    columns = shards * piece
    me = me_ref[0]
    hidden_copy = pltpu.make_async_copy(hidden_ref, hidden_buf, hidden_sem)
    hidden_copy.start()
    reads = [
        pltpu.make_async_copy(
            weights_ref.at[0, i * rows : (i + 1) * rows], weights_buf.at[i], in_sems.at[i]
        )
        for i in range(steps)
    ]
    for read in reads:
        read.start()
    hidden_copy.wait()
    depth = steps * rows
    for low in range(4):
        for high in range(4):
            for x, ref in ((0, keep_ref), (1, send_ref)):
                start = (me ^ (high * 8 + low * 2 + x)) * depth
                ref[low, high] = hidden_buf[:, pl.ds(pl.multiple_of(start, depth), depth)]
    writes = []
    for i in range(steps):
        reads[i].wait()
        for h in range(KVH):
            block = weights_buf[i, :, h * columns : (h + 1) * columns].astype(jnp.bfloat16)
            out_buf[i, :, :, h * rows : (h + 1) * rows] = block.T.reshape(shards, piece, rows)
        write = pltpu.make_async_copy(
            out_buf.at[i], out_ref.at[:, :, i * width : (i + 1) * width], out_sems.at[i]
        )
        write.start()
        writes.append(write)
    for write in writes:
        write.wait()


def enter(me, weights, hidden, shards):
    _, depth, columns = weights.shape
    piece = columns // KVH // shards
    steps = depth // ROW_TILE
    hbm = pl.BlockSpec(memory_space=pltpu.HBM)
    blocks = jax.ShapeDtypeStruct((4, 4, hidden.shape[0], depth), hidden.dtype)
    return pl.pallas_call(
        enter_kernel,
        in_specs=[pl.BlockSpec(memory_space=pltpu.SMEM), hbm, hbm],
        out_specs=[hbm, VMEM, VMEM],
        out_shape=[
            jax.ShapeDtypeStruct((shards, piece, KVH * depth), jnp.bfloat16), blocks, blocks
        ],
        scratch_shapes=[
            pltpu.VMEM((steps, ROW_TILE, columns), jnp.float32),
            pltpu.VMEM((steps, shards, piece, KVH * ROW_TILE), jnp.bfloat16),
            pltpu.VMEM(hidden.shape, hidden.dtype),
            pltpu.SemaphoreType.DMA((steps,)),
            pltpu.SemaphoreType.DMA((steps,)),
            pltpu.SemaphoreType.DMA,
        ],
        compiler_params=pltpu.CompilerParams(vmem_limit_bytes=63 * 1024 * 1024),
        cost_estimate=pl.CostEstimate(flops=2_000_000, bytes_accessed=3_000_000, transcendentals=0),
        name="enter",
    )(me, weights, hidden)


def pick_kernel(group_ref, spread_ref, out_ref):
    def move(s, carry):
        out_ref[group_ref[s]] = spread_ref[s]
        return carry

    lax.fori_loop(0, spread_ref.shape[0], move, 0)


def pick(section_to_group, spread):
    return pl.pallas_call(
        pick_kernel,
        in_specs=[pl.BlockSpec(memory_space=pltpu.SMEM), VMEM],
        out_specs=VMEM,
        out_shape=jax.ShapeDtypeStruct(spread.shape, spread.dtype),
        cost_estimate=pl.CostEstimate(flops=1_000_000, bytes_accessed=2_000_000, transcendentals=0),
        compiler_params=pltpu.CompilerParams(vmem_limit_bytes=12 * 1024 * 1024),
        name="pick",
    )(section_to_group, spread)


def multiply_kernel(me_ref, inputs_ref, routed_ref, out_ref, rows_ref):
    me = me_ref[0]
    shards, piece, width = routed_ref.shape
    heads, depth = KVH, width // KVH
    per_head = shards // heads
    own = inputs_ref.shape[1]
    block_rows = ROWS // per_head
    for d in range(shards):
        rows_ref[d * own : (d + 1) * own, :] = inputs_ref[me ^ d].astype(jnp.float32)
    inputs = rows_ref[...].astype(jnp.bfloat16)
    for h in range(heads):
        tiles = [
            routed_ref[:, :, (i * heads + h) * ROW_TILE : (i * heads + h + 1) * ROW_TILE]
            for i in range(depth // ROW_TILE)
        ]
        product = lax.dot_general(
            inputs,
            jnp.concatenate(tiles, axis=-1).reshape(shards * piece, depth),
            (((1,), (1,)), ((), ())),
            preferred_element_type=jnp.float32,
        )
        for i in range(per_head):
            r = me ^ (h * per_head + i)
            out_ref[r & 1, r >> 2, (r >> 1) & 1] = product[i * block_rows : (i + 1) * block_rows]


def multiply(me, inputs, routed):
    shards, _, width = routed.shape
    heads, depth = KVH, width // KVH
    return pl.pallas_call(
        multiply_kernel,
        in_specs=[pl.BlockSpec(memory_space=pltpu.SMEM), VMEM, VMEM],
        out_specs=VMEM,
        out_shape=jax.ShapeDtypeStruct((2, 8, 2, ROWS * heads // shards, 2 * HD), jnp.float32),
        scratch_shapes=[pltpu.VMEM((ROWS, depth), jnp.float32)],
        compiler_params=pltpu.CompilerParams(vmem_limit_bytes=12 * 1024 * 1024),
        cost_estimate=pl.CostEstimate(
            flops=2 * ROWS * heads * 2 * HD * depth, bytes_accessed=3_000_000, transcendentals=0
        ),
        name="multiply",
    )(me, inputs, routed)


def reduce_rows(partial):
    shards = lax.axis_size("shard")

    def send(values, bits):
        return lax.ppermute(values, "shard", [(i, i ^ bits) for i in range(shards)])

    partial = partial[0] + send(partial[1], 1)
    head = lax.reduce_precision(partial[1:], 8, 7)
    rest = partial[1:, :, :, :HD] - head[:, :, :, :HD]
    halves = jnp.concatenate([head, rest], axis=-1).astype(jnp.bfloat16)
    arrived = {}
    for k in (4, 5, 3, 6, 2, 7, 1):
        if k == 4:
            arrived[k] = send(halves[k - 1, ::-1], 9 << 1)
        else:
            arrived[k] = send(halves[k - 1], k << 2)
    total = sum(v.astype(jnp.float32) for v in arrived.values())
    keys = total[:, :, :HD] + total[:, :, 2 * HD :]
    partial = partial[0] + jnp.concatenate([keys, total[:, :, HD : 2 * HD]], axis=-1)
    partial = partial[0] + send(partial[1], 1 << 1)
    return partial


def step(train_weights, section_to_group, hidden, queries, kv_cache, lengths):
    shards = lax.axis_size("shard")
    sections = lax.axis_size("section")
    per_head = shards // KVH
    row_block = ROWS // per_head
    piece_cols = 2 * HD // shards
    slice_rows = train_weights.shape[1]
    me = lax.axis_index("shard").astype(jnp.int32).reshape(1)
    flipped, keep, other = enter(me, train_weights, hidden, shards)
    inputs = spread_rows(keep, other)
    flipped = flipped.reshape(sections, -1, KVH * slice_rows)
    spread = exchange(flipped, "section")
    picked = pick(section_to_group, spread)
    routed = exchange(picked, "section").reshape(shards, piece_cols, KVH * slice_rows)
    received = exchange(routed, "shard")
    layer_out = received.reshape(shards, piece_cols, -1, KVH, ROW_TILE)
    layer_out = layer_out.transpose(3, 1, 0, 2, 4).reshape(1, KVH, piece_cols, D)
    fresh = reduce_rows(multiply(me, inputs, routed)).astype(jnp.bfloat16)
    block_index = lax.axis_index("shard") % per_head
    row_lengths = lax.dynamic_slice_in_dim(lengths, block_index * row_block, row_block, 0)
    query_rows = queries.reshape(row_block, QPK, HD)
    context = attend(query_rows, kv_cache, fresh, row_lengths)
    return (context, layer_out)


def solution(mesh):
    return jax.shard_map(
        step,
        mesh=mesh,
        in_specs=(
            P("section", "shard", None),
            P(),
            P(("section", "shard"), None),
            P(("section", "shard"), None),
            P(("section", "shard"), None, None),
            P("section"),
        ),
        out_specs=(P(("section", "shard"), None), P("section", None, "shard", None)),
        check_vma=False,
    )
```

```python
import math

import jax
import jax.numpy as jnp
from jax import lax
from jax.experimental import pallas as pl
from jax.experimental.pallas import tpu as pltpu
from jax.sharding import PartitionSpec as P


D = 16384
HD = 128
QPK = 16
KVH = 4
LEN = 128
ROWS = 128
ROW_TILE = 128


def exchange(blocks, axis):
    return lax.all_to_all(blocks, axis, split_axis=0, concat_axis=0, tiled=True)


def spread_rows(keep, other):
    shards = lax.axis_size("shard")

    def send(values, bits):
        return lax.ppermute(values, "shard", [(i, i ^ bits) for i in range(shards)])

    side = [keep, send(other, 1)]
    near = [jnp.stack([v[k] for v in side]) for k in range(4)]
    near = [near[0]] + [send(near[k], k << 1) for k in range(1, 4)]
    far = [jnp.stack([v[:, k] for v in near]) for k in range(4)]
    for k in (2, 1, 3):
        far[k] = send(far[k], k << 3)
    return jnp.concatenate(far).reshape((shards,) + keep.shape[2:])


def attend(query_rows, cache_rows, fresh_rows, row_lengths):
    score_scale = 1.0 / math.sqrt(HD)
    cached_keys = cache_rows[:, :, :HD]
    cached_values = cache_rows[:, :, HD:]
    key_new = fresh_rows[:, :HD]
    value_new = fresh_rows[:, HD:]
    scores = (
        jnp.einsum("rhd,rtd->rht", query_rows, cached_keys, preferred_element_type=jnp.float32)
        * score_scale
    )
    valid = jnp.arange(LEN)[None, None, :] < row_lengths[:, None, None]
    scores = jnp.where(valid, scores, -1e30)
    fresh_score = (
        jnp.einsum("rhd,rd->rh", query_rows, key_new, preferred_element_type=jnp.float32)
        * score_scale
    )
    highest = jnp.maximum(jnp.max(scores, axis=-1), fresh_score)
    weights = jnp.where(valid, jnp.exp(scores - highest[..., None]), 0.0)
    fresh_weight = jnp.exp(fresh_score - highest)
    total = jnp.sum(weights, axis=-1) + fresh_weight
    probs = (weights / total[..., None]).astype(jnp.bfloat16)
    fresh_prob = (fresh_weight / total).astype(jnp.bfloat16)
    context = jnp.einsum("rht,rtd->rhd", probs, cached_values, preferred_element_type=jnp.float32)
    context = (
        context
        + fresh_prob.astype(jnp.float32)[..., None] * value_new.astype(jnp.float32)[:, None, :]
    )
    return context.reshape(context.shape[0], QPK * HD).astype(jnp.bfloat16)


VMEM = pl.BlockSpec(memory_space=pltpu.VMEM)


def enter_kernel(
    me_ref, weights_ref, hidden_ref, out_ref, keep_ref, send_ref,
    weights_buf, out_buf, hidden_buf, in_sems, out_sems, hidden_sem,
):
    steps, rows, _ = weights_buf.shape
    _, shards, piece, width = out_buf.shape
    columns = shards * piece
    me = me_ref[0]
    hidden_copy = pltpu.make_async_copy(hidden_ref, hidden_buf, hidden_sem)
    hidden_copy.start()
    reads = [
        pltpu.make_async_copy(
            weights_ref.at[0, i * rows : (i + 1) * rows], weights_buf.at[i], in_sems.at[i]
        )
        for i in range(steps)
    ]
    for read in reads:
        read.start()
    hidden_copy.wait()
    depth = steps * rows
    for low in range(4):
        for high in range(4):
            for x, ref in ((0, keep_ref), (1, send_ref)):
                start = (me ^ (high * 8 + low * 2 + x)) * depth
                ref[low, high] = hidden_buf[:, pl.ds(pl.multiple_of(start, depth), depth)]
    writes = []
    for i in range(steps):
        reads[i].wait()
        for h in range(KVH):
            block = weights_buf[i, :, h * columns : (h + 1) * columns].astype(jnp.bfloat16)
            out_buf[i, :, :, h * rows : (h + 1) * rows] = block.T.reshape(shards, piece, rows)
        write = pltpu.make_async_copy(
            out_buf.at[i], out_ref.at[:, :, i * width : (i + 1) * width], out_sems.at[i]
        )
        write.start()
        writes.append(write)
    for write in writes:
        write.wait()


def enter(me, weights, hidden, shards):
    _, depth, columns = weights.shape
    piece = columns // KVH // shards
    steps = depth // ROW_TILE
    hbm = pl.BlockSpec(memory_space=pltpu.HBM)
    blocks = jax.ShapeDtypeStruct((4, 4, hidden.shape[0], depth), hidden.dtype)
    return pl.pallas_call(
        enter_kernel,
        in_specs=[pl.BlockSpec(memory_space=pltpu.SMEM), hbm, hbm],
        out_specs=[hbm, VMEM, VMEM],
        out_shape=[
            jax.ShapeDtypeStruct((shards, piece, KVH * depth), jnp.bfloat16), blocks, blocks
        ],
        scratch_shapes=[
            pltpu.VMEM((steps, ROW_TILE, columns), jnp.float32),
            pltpu.VMEM((steps, shards, piece, KVH * ROW_TILE), jnp.bfloat16),
            pltpu.VMEM(hidden.shape, hidden.dtype),
            pltpu.SemaphoreType.DMA((steps,)),
            pltpu.SemaphoreType.DMA((steps,)),
            pltpu.SemaphoreType.DMA,
        ],
        compiler_params=pltpu.CompilerParams(vmem_limit_bytes=63 * 1024 * 1024),
        cost_estimate=pl.CostEstimate(flops=2_000_000, bytes_accessed=3_000_000, transcendentals=0),
        name="enter",
    )(me, weights, hidden)


def pick_kernel(group_ref, spread_ref, out_ref):
    def move(s, carry):
        out_ref[group_ref[s]] = spread_ref[s]
        return carry

    lax.fori_loop(0, spread_ref.shape[0], move, 0)


def pick(section_to_group, spread):
    return pl.pallas_call(
        pick_kernel,
        in_specs=[pl.BlockSpec(memory_space=pltpu.SMEM), VMEM],
        out_specs=VMEM,
        out_shape=jax.ShapeDtypeStruct(spread.shape, spread.dtype),
        cost_estimate=pl.CostEstimate(flops=1_000_000, bytes_accessed=2_000_000, transcendentals=0),
        compiler_params=pltpu.CompilerParams(vmem_limit_bytes=12 * 1024 * 1024),
        name="pick",
    )(section_to_group, spread)


def multiply_kernel(me_ref, inputs_ref, routed_ref, even_ref, odd_ref, rows_ref):
    me = me_ref[0]
    shards, piece, width = routed_ref.shape
    heads, depth = KVH, width // KVH
    per_head = shards // heads
    own = inputs_ref.shape[1]
    block_rows = ROWS // per_head
    for d in range(shards):
        rows_ref[d * own : (d + 1) * own, :] = inputs_ref[me ^ d].astype(jnp.float32)
    inputs = rows_ref[...].astype(jnp.bfloat16)
    for h in range(heads):
        tiles = [
            routed_ref[:, :, (i * heads + h) * ROW_TILE : (i * heads + h + 1) * ROW_TILE]
            for i in range(depth // ROW_TILE)
        ]
        product = lax.dot_general(
            inputs,
            jnp.concatenate(tiles, axis=-1).reshape(shards * piece, depth),
            (((1,), (1,)), ((), ())),
            preferred_element_type=jnp.float32,
        )
        for i in range(per_head):
            r = me ^ (h * per_head + i)
            value = product[i * block_rows : (i + 1) * block_rows]
            own_side = (r & 1) == 0

            @pl.when(own_side)
            def _():
                even_ref[r >> 2, (r >> 1) & 1] = value

            @pl.when(jnp.logical_not(own_side))
            def _():
                odd_ref[r >> 2, (r >> 1) & 1] = value


def multiply(me, inputs, routed):
    shards, _, width = routed.shape
    heads, depth = KVH, width // KVH
    return pl.pallas_call(
        multiply_kernel,
        in_specs=[pl.BlockSpec(memory_space=pltpu.SMEM), VMEM, VMEM],
        out_specs=[VMEM, VMEM],
        out_shape=[jax.ShapeDtypeStruct((8, 2, ROWS * heads // shards, 2 * HD), jnp.float32)] * 2,
        scratch_shapes=[pltpu.VMEM((ROWS, depth), jnp.float32)],
        compiler_params=pltpu.CompilerParams(vmem_limit_bytes=12 * 1024 * 1024),
        cost_estimate=pl.CostEstimate(
            flops=2 * ROWS * heads * 2 * HD * depth, bytes_accessed=3_000_000, transcendentals=0
        ),
        name="multiply",
    )(me, inputs, routed)


def reduce_rows(even, odd):
    shards = lax.axis_size("shard")

    def send(values, bits):
        return lax.ppermute(values, "shard", [(i, i ^ bits) for i in range(shards)])

    partial = even + send(odd, 1)
    head = lax.reduce_precision(partial[1:], 8, 7)
    rest = partial[1:, :, :, :HD] - head[:, :, :, :HD]
    halves = jnp.concatenate([head, rest], axis=-1).astype(jnp.bfloat16)
    arrived = {}
    for k in (4, 5, 3, 6, 2, 7, 1):
        arrived[k] = send(halves[k - 1], k << 2)
    total = sum(v.astype(jnp.float32) for v in arrived.values())
    keys = total[:, :, :HD] + total[:, :, 2 * HD :]
    partial = partial[0] + jnp.concatenate([keys, total[:, :, HD : 2 * HD]], axis=-1)
    partial = partial[0] + send(partial[1], 1 << 1)
    return partial


def step(train_weights, section_to_group, hidden, queries, kv_cache, lengths):
    shards = lax.axis_size("shard")
    sections = lax.axis_size("section")
    per_head = shards // KVH
    row_block = ROWS // per_head
    piece_cols = 2 * HD // shards
    slice_rows = train_weights.shape[1]
    me = lax.axis_index("shard").astype(jnp.int32).reshape(1)
    flipped, keep, other = enter(me, train_weights, hidden, shards)
    inputs = spread_rows(keep, other)
    flipped = flipped.reshape(sections, -1, KVH * slice_rows)
    spread = exchange(flipped, "section")
    picked = pick(section_to_group, spread)
    routed = exchange(picked, "section").reshape(shards, piece_cols, KVH * slice_rows)
    received = exchange(routed, "shard")
    layer_out = received.reshape(shards, piece_cols, -1, KVH, ROW_TILE)
    layer_out = layer_out.transpose(3, 1, 0, 2, 4).reshape(1, KVH, piece_cols, D)
    fresh = reduce_rows(*multiply(me, inputs, routed)).astype(jnp.bfloat16)
    block_index = lax.axis_index("shard") % per_head
    row_lengths = lax.dynamic_slice_in_dim(lengths, block_index * row_block, row_block, 0)
    query_rows = queries.reshape(row_block, QPK, HD)
    context = attend(query_rows, kv_cache, fresh, row_lengths)
    return (context, layer_out)


def solution(mesh):
    return jax.shard_map(
        step,
        mesh=mesh,
        in_specs=(
            P("section", "shard", None),
            P(),
            P(("section", "shard"), None),
            P(("section", "shard"), None),
            P(("section", "shard"), None, None),
            P("section"),
        ),
        out_specs=(P(("section", "shard"), None), P("section", None, "shard", None)),
        check_vma=False,
    )
```

```python
import math

import jax
import jax.numpy as jnp
from jax import lax
from jax.experimental import pallas as pl
from jax.experimental.pallas import tpu as pltpu
from jax.sharding import PartitionSpec as P


D = 16384
HD = 128
QPK = 16
KVH = 4
LEN = 128
ROWS = 128
ROW_TILE = 128


def exchange(blocks, axis):
    return lax.all_to_all(blocks, axis, split_axis=0, concat_axis=0, tiled=True)


def spread_rows(keep, other):
    shards = lax.axis_size("shard")

    def send(values, bits):
        return lax.ppermute(values, "shard", [(i, i ^ bits) for i in range(shards)])

    side = [keep, send(other, 1)]
    near = [jnp.stack([v[k] for v in side]) for k in range(4)]
    near = [near[0]] + [send(near[k], k << 1) for k in range(1, 4)]
    far = [jnp.stack([v[:, k] for v in near]) for k in range(4)]
    for k in (1, 2, 3):
        far[k] = send(far[k], k << 3)
    return jnp.concatenate(far).reshape((shards,) + keep.shape[2:])


def attend(query_rows, cache_rows, fresh_rows, row_lengths):
    score_scale = 1.0 / math.sqrt(HD)
    cached_keys = cache_rows[:, :, :HD]
    cached_values = cache_rows[:, :, HD:]
    key_new = fresh_rows[:, :HD]
    value_new = fresh_rows[:, HD:]
    scores = (
        jnp.einsum("rhd,rtd->rht", query_rows, cached_keys, preferred_element_type=jnp.float32)
        * score_scale
    )
    valid = jnp.arange(LEN)[None, None, :] < row_lengths[:, None, None]
    scores = jnp.where(valid, scores, -1e30)
    fresh_score = (
        jnp.einsum("rhd,rd->rh", query_rows, key_new, preferred_element_type=jnp.float32)
        * score_scale
    )
    highest = jnp.maximum(jnp.max(scores, axis=-1), fresh_score)
    weights = jnp.where(valid, jnp.exp(scores - highest[..., None]), 0.0)
    fresh_weight = jnp.exp(fresh_score - highest)
    total = jnp.sum(weights, axis=-1) + fresh_weight
    probs = (weights / total[..., None]).astype(jnp.bfloat16)
    fresh_prob = (fresh_weight / total).astype(jnp.bfloat16)
    context = jnp.einsum("rht,rtd->rhd", probs, cached_values, preferred_element_type=jnp.float32)
    context = (
        context
        + fresh_prob.astype(jnp.float32)[..., None] * value_new.astype(jnp.float32)[:, None, :]
    )
    return context.reshape(context.shape[0], QPK * HD).astype(jnp.bfloat16)


VMEM = pl.BlockSpec(memory_space=pltpu.VMEM)


def enter_kernel(
    me_ref, weights_ref, hidden_ref, out_ref, keep_ref, send_ref,
    weights_buf, out_buf, hidden_buf, in_sems, out_sems, hidden_sem,
):
    steps, rows, _ = weights_buf.shape
    _, shards, piece, width = out_buf.shape
    columns = shards * piece
    me = me_ref[0]
    hidden_copy = pltpu.make_async_copy(hidden_ref, hidden_buf, hidden_sem)
    hidden_copy.start()
    reads = [
        pltpu.make_async_copy(
            weights_ref.at[0, i * rows : (i + 1) * rows], weights_buf.at[i], in_sems.at[i]
        )
        for i in range(steps)
    ]
    for read in reads:
        read.start()
    hidden_copy.wait()
    depth = steps * rows
    for low in range(4):
        for high in range(4):
            for x, ref in ((0, keep_ref), (1, send_ref)):
                start = (me ^ (high * 8 + low * 2 + x)) * depth
                ref[low, high] = hidden_buf[:, pl.ds(pl.multiple_of(start, depth), depth)]
    writes = []
    for i in range(steps):
        reads[i].wait()
        for h in range(KVH):
            block = weights_buf[i, :, h * columns : (h + 1) * columns].astype(jnp.bfloat16)
            out_buf[i, :, :, h * rows : (h + 1) * rows] = block.T.reshape(shards, piece, rows)
        write = pltpu.make_async_copy(
            out_buf.at[i], out_ref.at[:, :, i * width : (i + 1) * width], out_sems.at[i]
        )
        write.start()
        writes.append(write)
    for write in writes:
        write.wait()


def enter(me, weights, hidden, shards):
    _, depth, columns = weights.shape
    piece = columns // KVH // shards
    steps = depth // ROW_TILE
    hbm = pl.BlockSpec(memory_space=pltpu.HBM)
    blocks = jax.ShapeDtypeStruct((4, 4, hidden.shape[0], depth), hidden.dtype)
    return pl.pallas_call(
        enter_kernel,
        in_specs=[pl.BlockSpec(memory_space=pltpu.SMEM), hbm, hbm],
        out_specs=[hbm, VMEM, VMEM],
        out_shape=[
            jax.ShapeDtypeStruct((shards, piece, KVH * depth), jnp.bfloat16), blocks, blocks
        ],
        scratch_shapes=[
            pltpu.VMEM((steps, ROW_TILE, columns), jnp.float32),
            pltpu.VMEM((steps, shards, piece, KVH * ROW_TILE), jnp.bfloat16),
            pltpu.VMEM(hidden.shape, hidden.dtype),
            pltpu.SemaphoreType.DMA((steps,)),
            pltpu.SemaphoreType.DMA((steps,)),
            pltpu.SemaphoreType.DMA,
        ],
        compiler_params=pltpu.CompilerParams(vmem_limit_bytes=63 * 1024 * 1024),
        cost_estimate=pl.CostEstimate(flops=2_000_000, bytes_accessed=3_000_000, transcendentals=0),
        name="enter",
    )(me, weights, hidden)


def pick_kernel(group_ref, spread_ref, out_ref):
    def move(s, carry):
        out_ref[group_ref[s]] = spread_ref[s]
        return carry

    lax.fori_loop(0, spread_ref.shape[0], move, 0)


def pick(section_to_group, spread):
    return pl.pallas_call(
        pick_kernel,
        in_specs=[pl.BlockSpec(memory_space=pltpu.SMEM), VMEM],
        out_specs=VMEM,
        out_shape=jax.ShapeDtypeStruct(spread.shape, spread.dtype),
        cost_estimate=pl.CostEstimate(flops=1_000_000, bytes_accessed=2_000_000, transcendentals=0),
        compiler_params=pltpu.CompilerParams(vmem_limit_bytes=12 * 1024 * 1024),
        name="pick",
    )(section_to_group, spread)


def multiply_kernel(me_ref, inputs_ref, routed_ref, out_ref, rows_ref):
    me = me_ref[0]
    shards, piece, width = routed_ref.shape
    heads, depth = KVH, width // KVH
    per_head = shards // heads
    own = inputs_ref.shape[1]
    block_rows = ROWS // per_head
    for d in range(shards):
        rows_ref[d * own : (d + 1) * own, :] = inputs_ref[me ^ d].astype(jnp.float32)
    inputs = rows_ref[...].astype(jnp.bfloat16)
    for h in range(heads):
        tiles = [
            routed_ref[:, :, (i * heads + h) * ROW_TILE : (i * heads + h + 1) * ROW_TILE]
            for i in range(depth // ROW_TILE)
        ]
        product = lax.dot_general(
            inputs,
            jnp.concatenate(tiles, axis=-1).reshape(shards * piece, depth),
            (((1,), (1,)), ((), ())),
            preferred_element_type=jnp.float32,
        )
        for i in range(per_head):
            r = me ^ (h * per_head + i)
            out_ref[r & 1, r >> 2, (r >> 1) & 1] = product[i * block_rows : (i + 1) * block_rows]


def multiply(me, inputs, routed):
    shards, _, width = routed.shape
    heads, depth = KVH, width // KVH
    return pl.pallas_call(
        multiply_kernel,
        in_specs=[pl.BlockSpec(memory_space=pltpu.SMEM), VMEM, VMEM],
        out_specs=VMEM,
        out_shape=jax.ShapeDtypeStruct((2, 8, 2, ROWS * heads // shards, 2 * HD), jnp.float32),
        scratch_shapes=[pltpu.VMEM((ROWS, depth), jnp.float32)],
        compiler_params=pltpu.CompilerParams(vmem_limit_bytes=12 * 1024 * 1024),
        cost_estimate=pl.CostEstimate(
            flops=2 * ROWS * heads * 2 * HD * depth, bytes_accessed=3_000_000, transcendentals=0
        ),
        name="multiply",
    )(me, inputs, routed)


def reduce_rows(partial):
    shards = lax.axis_size("shard")

    def send(values, bits):
        return lax.ppermute(values, "shard", [(i, i ^ bits) for i in range(shards)])

    partial = partial[0] + send(partial[1], 1)
    head = lax.reduce_precision(partial[1:], 8, 7)
    rest = partial[1:, :, :, :HD] - head[:, :, :, :HD]
    halves = jnp.concatenate([head, rest], axis=-1).astype(jnp.bfloat16)
    arrived = {}
    for k in (4, 5, 3, 6, 2, 7, 1):
        arrived[k] = send(halves[k - 1], k << 2)
    total = sum(v.astype(jnp.float32) for v in arrived.values())
    keys = total[:, :, :HD] + total[:, :, 2 * HD :]
    partial = partial[0] + jnp.concatenate([keys, total[:, :, HD : 2 * HD]], axis=-1)
    partial = partial[0] + send(partial[1], 1 << 1)
    return partial


def step(train_weights, section_to_group, hidden, queries, kv_cache, lengths):
    shards = lax.axis_size("shard")
    sections = lax.axis_size("section")
    per_head = shards // KVH
    row_block = ROWS // per_head
    piece_cols = 2 * HD // shards
    slice_rows = train_weights.shape[1]
    me = lax.axis_index("shard").astype(jnp.int32).reshape(1)
    flipped, keep, other = enter(me, train_weights, hidden, shards)
    inputs = spread_rows(keep, other)
    flipped = flipped.reshape(sections, -1, KVH * slice_rows)
    spread = exchange(flipped, "section")
    picked = pick(section_to_group, spread)
    routed = exchange(picked, "section").reshape(shards, piece_cols, KVH * slice_rows)
    received = exchange(routed, "shard")
    layer_out = received.reshape(shards, piece_cols, -1, KVH, ROW_TILE)
    layer_out = layer_out.transpose(3, 1, 0, 2, 4).reshape(1, KVH, piece_cols, D)
    fresh = reduce_rows(multiply(me, inputs, routed)).astype(jnp.bfloat16)
    block_index = lax.axis_index("shard") % per_head
    row_lengths = lax.dynamic_slice_in_dim(lengths, block_index * row_block, row_block, 0)
    query_rows = queries.reshape(row_block, QPK, HD)
    context = attend(query_rows, kv_cache, fresh, row_lengths)
    return (context, layer_out)


def solution(mesh):
    return jax.shard_map(
        step,
        mesh=mesh,
        in_specs=(
            P("section", "shard", None),
            P(),
            P(("section", "shard"), None),
            P(("section", "shard"), None),
            P(("section", "shard"), None, None),
            P("section"),
        ),
        out_specs=(P(("section", "shard"), None), P("section", None, "shard", None)),
        check_vma=False,
    )
```
